1024 devices in a mesh: grp: 16 (over x, z_hi), seq: 16 (over z_lo, core), tp: 4 (over y).
Axes of the slice: x: 4, y: 4, z: 32 (z_hi: 4, z_lo: 8; z = z_hi * 8 + z_lo), core: 2. Of those that a mesh axis runs over, the one named last changes fastest.
Arguments:
- hidden: bfloat16 [32768, 8192], P(('grp', 'seq')), may hold values from -6 to 6
- queries: bfloat16 [32768, 4096], P(('grp', 'seq'), 'tp'), may hold values from -900 to 900, as said below
- vis_rows: bfloat16 [256, 16, 4, 8192], P(('grp', 'seq')), may hold values from -6 to 6
- vis_slot: int32 [256, 16, 4], P(('grp', 'seq')), may hold values from -1 to 127, as said below
- doc_ids: int32 [16, 2048], P('grp', 'seq'), may hold values from 0 to 7, never falling along the last dimension, each value on 1 to 1024 neighbouring positions
- w_key: bfloat16 [8192, 512], P('grp', 'tp'), may hold values from -0.0625 to 0.0625
- w_value: bfloat16 [8192, 512], P('grp', 'tp'), may hold values from -0.0625 to 0.0625
Outputs:
- attended: bfloat16 [32768, 4096], P(('grp', 'seq'), 'tp')
The draws below stay inside these ranges and needn't reach their ends.
Inputs may be any that keep to these rules, and one draw needn't show every extreme that they name: `queries`: a row may be scaled far from one. `vis_slot`: entry [g * 16 + s, d, c] names a position within the 128 positions of index d of seq in group g, or -1. Live positions are distinct within a destination; each device sends 1 to 4 live rows to every destination, slots 0 upward; in every group one destination receives 4 from every device.
All inputs are finite; a program needn't handle non-finite values.
Results may differ from the reference program's by a relative error of at most 0.024.
Values may be sent and summed in bfloat16 or wider, within the bound.
No kernel may reach another device: no remote copies, remote signals or barrier semaphores. Data moves between devices by JAX's collectives and lax.ppermute only.
A program may use at most 32 MiB of HBM per device.

```python
import math
import jax
import jax.numpy as jnp
import numpy as np
from jax import lax

D = 8192
HEAD = 128
KVH = 4
QPK = 8
TOK_DEV = 128
CAP = 4
LEN = 2048
GROUPS = 16
N_SEQ = 16


def draw_queries(key, part):
    first = jax.random.fold_in(jax.random.fold_in(key, 11), 0)
    base = jnp.clip(jax.random.normal(first, (GROUPS * LEN, KVH * QPK * HEAD), jnp.float32), -6.0, 6.0)
    return base.astype(jnp.bfloat16)


def draw_vis_slot(key, part):
    first, second, third = jax.random.split(jax.random.fold_in(key, 23), 3)
    orders = jax.vmap(lambda one: jax.random.permutation(one, TOK_DEV))(jax.random.split(first, GROUPS * N_SEQ))
    taken = orders[:, :N_SEQ * CAP].reshape(GROUPS, N_SEQ, N_SEQ, CAP).transpose(0, 2, 1, 3)
    counts = jax.random.randint(second, (GROUPS, N_SEQ, N_SEQ), 1, CAP + 1)
    filled = jax.random.randint(third, (GROUPS, 1, 1), 0, N_SEQ)
    target = lax.broadcasted_iota(jnp.int32, (GROUPS, N_SEQ, N_SEQ), 2)
    counts = jnp.where(target == filled, CAP, counts)
    place = lax.broadcasted_iota(jnp.int32, (GROUPS, N_SEQ, N_SEQ, CAP), 3)
    slots = jnp.where(place < counts[..., None], taken, -1)
    return slots.reshape(GROUPS * N_SEQ, N_SEQ, CAP).astype(jnp.int32)


def block_levels(own_key, extent, cuts, least, top_value):
    level = 1.0
    for axis_at, blocks in cuts:
        steps = jax.random.uniform(jax.random.fold_in(jax.random.fold_in(own_key, 6), axis_at), (blocks,), jnp.float32, least / len(cuts), top_value / len(cuts))
        level = level * jnp.repeat(jnp.exp(steps), extent[axis_at] // blocks).reshape((-1,) + (1,) * (len(extent) - 1 - axis_at))
    return level


def length_profile(count, total, limit, lean):
    weights = [(1 << 20) // math.isqrt(rank ** lean) + 1 for rank in range(2, count + 1)]
    surplus, given = total - limit - (count - 1), [1] * (count - 1)
    while surplus > 0:
        free = [i for i in range(count - 1) if given[i] < limit]
        pool, remaining = sum([weights[i] for i in free]), surplus
        for i in free:
            more = min(limit - given[i], max(1, remaining * weights[i] // pool), surplus)
            given[i] = given[i] + more
            surplus = surplus - more
    return np.array([limit] + given)


def ragged_sizes(key, amount, total, reach, lean):
    if amount == 2:
        one = jax.random.randint(key, (), max(1, total - reach), min(reach, total - 1) + 1)
        return jnp.stack([one, total - one])
    tallies = jnp.asarray(length_profile(amount, total, reach, lean), jnp.int32)
    couples = (amount - 1) // 2
    source_of, sink = tallies[1:1 + 2 * couples:2], tallies[2:2 + 2 * couples:2]
    room = jnp.minimum(source_of - 1, reach - sink)
    shifted = jax.random.randint(jax.random.fold_in(key, 1), (couples,), 0, 1 << 20) % (room + 1)
    tallies = tallies.at[1:1 + 2 * couples:2].set(source_of - shifted).at[2:2 + 2 * couples:2].set(sink + shifted)
    return tallies[jax.random.permutation(jax.random.fold_in(key, 2), amount)]


def centred(stream_key, dims, width, reach, cuts=(), kind=jnp.bfloat16):
    drawn = width * jax.random.normal(stream_key, dims, jnp.float32)
    if cuts:
        drawn = drawn * block_levels(stream_key, dims, cuts, -0.22, 0.18)
    return jnp.clip(drawn, -reach, reach).astype(kind)


def setup_inputs(seed: int = 0) -> dict:
    arg_keys = jax.random.split(jax.random.key(seed), 8)
    return {
        "hidden": centred(arg_keys[0], (GROUPS * LEN, D), 1.0, 6.0, ((0, 256),)),
        "queries": draw_queries(jax.random.fold_in(arg_keys[7], 71), 0),
        "vis_rows": centred(arg_keys[2], (GROUPS * N_SEQ, N_SEQ, CAP, D), 1.0, 6.0, ((0, 256),)),
        "vis_slot": draw_vis_slot(jax.random.fold_in(arg_keys[7], 71), 0),
        "doc_ids": jax.vmap(lambda own: jnp.searchsorted(jnp.cumsum(ragged_sizes(own, 8, LEN, LEN // 2, 2)), jnp.arange(LEN), side="right"))(jax.random.split(arg_keys[4], GROUPS)).reshape((GROUPS, LEN)).astype(jnp.int32),
        "w_key": centred(arg_keys[5], (D, KVH * HEAD), D ** -0.5, 0.0625, ((0, 16), (1, 4))),
        "w_value": centred(arg_keys[6], (D, KVH * HEAD), D ** -0.5, 0.0625, ((0, 16), (1, 4))),
    }


def head_attend(q_head, key, value, allowed):
    scores = jnp.dot(q_head, key.T, preferred_element_type=jnp.float32) / jnp.sqrt(jnp.float32(HEAD))
    scores = jnp.where(allowed, scores, jnp.float32(-1e+30))
    top = lax.optimization_barrier(jnp.max(scores, axis=1, keepdims=True))
    weights = jnp.where(allowed, jnp.exp(scores - top), jnp.float32(0.0))
    total = lax.optimization_barrier(jnp.sum(weights, axis=1, keepdims=True))
    mixed = jnp.dot(weights.astype(jnp.bfloat16), value, preferred_element_type=jnp.float32)
    return (mixed / total).astype(jnp.bfloat16)

def one_group(inputs, w_key, w_value):
    hidden, queries, rows, slots, docs = inputs
    text_keys = jnp.dot(hidden, w_key, preferred_element_type=jnp.float32).astype(jnp.bfloat16)
    text_values = jnp.dot(hidden, w_value, preferred_element_type=jnp.float32).astype(jnp.bfloat16)
    flat = rows.reshape(-1, D)
    vis_keys = jnp.dot(flat, w_key, preferred_element_type=jnp.float32).astype(jnp.bfloat16)
    vis_values = jnp.dot(flat, w_value, preferred_element_type=jnp.float32).astype(jnp.bfloat16)
    target = lax.broadcasted_iota(jnp.int32, slots.shape, 1)
    where_to = jnp.where(slots >= 0, target * TOK_DEV + slots, LEN).reshape(-1).astype(jnp.int32)
    keys = text_keys.at[where_to].set(vis_keys, mode='drop')
    values = text_values.at[where_to].set(vis_values, mode='drop')
    places = jnp.arange(LEN, dtype=jnp.int32)
    allowed = (places[None, :] <= places[:, None]) & (docs[None, :] == docs[:, None])
    q_heads = queries.reshape(LEN, KVH, QPK, HEAD).transpose(1, 2, 0, 3)
    k_heads = keys.reshape(LEN, KVH, HEAD).transpose(1, 0, 2)
    v_heads = values.reshape(LEN, KVH, HEAD).transpose(1, 0, 2)

    def per_kv(items):
        q_group, key, value = items
        return lax.map(lambda q_head: head_attend(q_head, key, value, allowed), q_group)
    out = lax.map(per_kv, (q_heads, k_heads, v_heads))
    return out.transpose(2, 0, 1, 3).reshape(LEN, KVH * QPK * HEAD)

def reference(hidden, queries, vis_rows, vis_slot, doc_ids, w_key, w_value):
    stacked = (hidden.reshape(GROUPS, LEN, D), queries.reshape(GROUPS, LEN, KVH * QPK * HEAD), vis_rows.reshape(GROUPS, N_SEQ, N_SEQ, CAP, D), vis_slot.reshape(GROUPS, N_SEQ, N_SEQ, CAP), doc_ids)
    out = lax.map(lambda items: one_group(items, w_key, w_value), stacked)
    return out.reshape(GROUPS * LEN, KVH * QPK * HEAD)
```

```python
import jax
import jax.numpy as jnp
from jax import lax
from jax.experimental import pallas as pl
from jax.experimental.pallas import tpu as pltpu
from jax.sharding import PartitionSpec as P


HEAD = 128
QPK = 8
CAP = 4
NX = 4
NZ = 4
NLO = 8
NS = 16
NT = 4
REACH = 4
AXES = ("grp", "seq", "tp")
OVER_X = [[x * NZ + z for x in range(NX)] for z in range(NZ)]
OVER_Z = [[x * NZ + z for z in range(NZ)] for x in range(NX)]


def seq_permute(array, move):
    pairs = []
    for g in range(NX * NZ):
        for s in range(NS):
            to = move(s // 2, s % 2)
            if to is None:
                continue
            for t in range(NT):
                pairs.append(((g * NS + s) * NT + t, (g * NS + to[0] * 2 + to[1]) * NT + t))
    return lax.ppermute(array, AXES, pairs)


def x_permute(array, d):
    step, size = NZ * NS * NT, NX * NZ * NS * NT
    return lax.ppermute(array, AXES, [(i, (i + d * step) % size) for i in range(size)])


def sibling(z, c):
    return z, 1 - c


def flip(mask):
    return lambda z, c: (z ^ mask, c)


def later(d):
    return lambda z, c: (z + d, c) if z + d < NLO else None


MIB = 1 << 20
IN_VMEM = pl.BlockSpec(memory_space=pltpu.VMEM)


def in_vmem(array):
    return pltpu.with_memory_space_constraint(array, pltpu.VMEM)


def pack(_, text_ref, extra_ref, out_ref):
    tokens = text_ref.shape[0]
    out_ref[:tokens, :] = text_ref[...]
    out_ref[tokens:, :] = extra_ref[...]


def packed(which, hidden, extra):
    tokens, width = hidden.shape
    count = tokens + extra.shape[0]
    part = width // NX
    return pl.pallas_call(
        pack,
        grid_spec=pltpu.PrefetchScalarGridSpec(
            num_scalar_prefetch=1,
            grid=(1,),
            in_specs=[
                pl.BlockSpec((tokens, part), lambda i, at: (0, at[0])),
                pl.BlockSpec((extra.shape[0], part), lambda i, at: (0, at[0])),
            ],
            out_specs=IN_VMEM,
        ),
        out_shape=pltpu.VMEM((count, part), hidden.dtype),
        compiler_params=pltpu.CompilerParams(vmem_limit_bytes=8 * MIB),
        name="pack",
    )(which, hidden, extra)


def project(place_ref, text_ref, extra_ref, *refs):
    *moved_refs, mine_ref, other_ref, out_ref, weights_ref = refs
    steps, sources, part, cols = mine_ref.shape
    tokens = text_ref.shape[0]
    s, x = place_ref[0], place_ref[1]
    core, chip = lax.rem(s, 2), lax.rem(s // 2, 4)
    for side, ref in enumerate((mine_ref, other_ref)):
        at = pl.ds(pl.multiple_of(jnp.where(core == side, 0, cols), cols), cols)
        for k in range(steps):
            piece = 2 * lax.rem(chip // 2 + k // 2, 2) + lax.rem(chip + k % 2, 2)
            for z in range(sources):
                row = pl.ds(pl.multiple_of(z * steps * part + piece * part, part), part)
                weights_ref[row, at] = ref[k, z]
    weights = weights_ref[...]
    out_ref[x, :tokens, :] = jnp.dot(text_ref[...], weights, preferred_element_type=jnp.float32)
    out_ref[x, tokens:, :] = jnp.dot(extra_ref[...], weights, preferred_element_type=jnp.float32)
    for d, ref in enumerate(moved_refs, 1):
        out_ref[lax.rem(x + NX - d, NX)] = jnp.dot(
            ref[...], weights, preferred_element_type=jnp.float32
        )


def projection(place, hidden, extra, moved, mine, other):
    tokens, width = hidden.shape
    count = tokens + extra.shape[0]
    part = width // NX
    cols = 2 * mine.shape[-1]
    return pl.pallas_call(
        project,
        grid_spec=pltpu.PrefetchScalarGridSpec(
            num_scalar_prefetch=1,
            grid=(1,),
            in_specs=[
                pl.BlockSpec((tokens, part), lambda i, at: (0, at[1])),
                pl.BlockSpec((extra.shape[0], part), lambda i, at: (0, at[1])),
            ]
            + [IN_VMEM] * (len(moved) + 2),
            out_specs=IN_VMEM,
            scratch_shapes=[pltpu.VMEM((part, cols), jnp.bfloat16)],
        ),
        out_shape=pltpu.VMEM((NX, count, cols), jnp.float32),
        compiler_params=pltpu.CompilerParams(vmem_limit_bytes=16 * MIB),
        name="project",
    )(place, hidden, extra, *map(in_vmem, (*moved, mine, other)))


def merge(sums_ref, vis_ref, docs_ref, out_ref):
    tokens, cols = sums_ref.shape[1:]
    text = jnp.sum(sums_ref[...], axis=0)
    slots = vis_ref[:, cols:].astype(jnp.float32)
    matches = slots == lax.broadcasted_iota(jnp.int32, slots.shape, 1).astype(jnp.float32)
    chooser = matches.astype(jnp.float32).astype(jnp.bfloat16)
    dims = (((0,), (0,)), ((), ()))
    moved = lax.dot_general(chooser, vis_ref[:, :cols], dims, preferred_element_type=jnp.float32)
    ones = jnp.ones((slots.shape[0], cols), jnp.bfloat16)
    used = lax.dot_general(chooser, ones, dims, preferred_element_type=jnp.float32)
    out_ref[:tokens, :] = jnp.where(used > 0.5, moved, text).astype(jnp.bfloat16)
    out_ref[tokens:, :] = docs_ref[...]


def merged_block(sums, vis, docs):
    _, tokens, cols = sums.shape
    extra = docs.shape[0]
    return pl.pallas_call(
        merge,
        in_specs=[IN_VMEM] * 3,
        out_specs=IN_VMEM,
        out_shape=pltpu.VMEM((tokens + extra, cols), jnp.bfloat16),
        compiler_params=pltpu.CompilerParams(vmem_limit_bytes=8 * MIB),
        name="merge",
    )(in_vmem(sums), in_vmem(vis), docs)


def attend(place_ref, q_ref, mine_ref, other_ref, my_docs_ref, out_ref, bias_ref, keys_ref, values_ref):
    tokens = q_ref.shape[0]
    blocks = mine_ref.shape[0]

    @pl.when(pl.program_id(0) == 0)
    def _():
        s = place_ref[0]
        core, chip = lax.rem(s, 2), s // 2
        my_docs = jnp.broadcast_to(my_docs_ref[...], (tokens, tokens))
        row = lax.broadcasted_iota(jnp.int32, (tokens, tokens), 0) + s * tokens
        col = lax.broadcasted_iota(jnp.int32, (tokens, tokens), 1)
        for side, ref in enumerate((mine_ref, other_ref)):
            for d in range(blocks):
                block = 2 * (chip - d) + (core if side == 0 else 1 - core)
                docs = ref[d, tokens : tokens + 8, :tokens].astype(jnp.float32)[:1]
                spot = col + block * tokens
                allowed = (docs == my_docs) & (spot <= row) & (spot >= 0)
                at = (side * blocks + d) * tokens
                bias_ref[:, at : at + tokens] = jnp.where(allowed, 0.0, -1e30)
                keys_ref[at : at + tokens, :] = ref[d, :tokens, :HEAD]
                values_ref[at : at + tokens, :] = ref[d, :tokens, HEAD:]

    scale = 1.0 / jnp.sqrt(jnp.float32(HEAD))
    scores = lax.dot_general(
        q_ref[...], keys_ref[...], (((1,), (1,)), ((), ())), preferred_element_type=jnp.float32
    )
    scores = scores * scale + bias_ref[...]
    top = jnp.max(scores, axis=1, keepdims=True)
    weights = jnp.exp(scores - top)
    total = jnp.sum(weights, axis=1, keepdims=True)
    mixed = jnp.dot(weights.astype(jnp.bfloat16), values_ref[...], preferred_element_type=jnp.float32)
    out_ref[...] = (mixed / total).astype(out_ref.dtype)


def attention(place, queries, mine, other, my_docs):
    tokens = queries.shape[0]
    span = 2 * mine.shape[0] * tokens
    return pl.pallas_call(
        attend,
        grid_spec=pltpu.PrefetchScalarGridSpec(
            num_scalar_prefetch=1,
            grid=(QPK,),
            in_specs=[
                pl.BlockSpec((tokens, HEAD), lambda h, *_: (0, h)),
                IN_VMEM,
                IN_VMEM,
                IN_VMEM,
            ],
            out_specs=pl.BlockSpec((tokens, HEAD), lambda h, *_: (0, h)),
            scratch_shapes=[
                pltpu.VMEM((tokens, span), jnp.float32),
                pltpu.VMEM((span, HEAD), jnp.bfloat16),
                pltpu.VMEM((span, HEAD), jnp.bfloat16),
            ],
        ),
        out_shape=jax.ShapeDtypeStruct(queries.shape, jnp.bfloat16),
        compiler_params=pltpu.CompilerParams(vmem_limit_bytes=16 * MIB),
        name="attend",
    )(place, queries, in_vmem(mine), in_vmem(other), my_docs)


def exchange_x(array):
    return lax.all_to_all(array, "grp", 0, 0, axis_index_groups=OVER_X, tiled=True)


def program(hidden, queries, vis_rows, vis_slot, doc_ids, w_key, w_value):
    tokens, width = hidden.shape
    cols = 2 * w_key.shape[1]
    place = lax.axis_index("seq")
    core, chip = place % 2, place // 2
    x = lax.axis_index("grp") // NZ
    where = jnp.stack([place, x])

    part = w_key.shape[0] // 4
    start = (chip % 4) * part
    piece = jnp.where(
        core == 0,
        lax.dynamic_slice_in_dim(w_key, start, part, axis=0),
        lax.dynamic_slice_in_dim(w_value, start, part, axis=0),
    )
    got = lax.all_to_all(
        jnp.broadcast_to(piece, (NZ, *piece.shape)), "grp", 0, 0, axis_index_groups=OVER_Z, tiled=True
    )

    extra = vis_rows.reshape(-1, width)
    moved = {}
    for d in (2, 1, 3):
        part_d = packed(((x + d) % NX).reshape(1), hidden, extra)
        moved[d] = x_permute(part_d, d)

    near = seq_permute(got, flip(1))
    pair = jnp.stack([got, near])
    far = seq_permute(pair, flip(2))
    four = jnp.concatenate([pair, far])
    rest = seq_permute(four, sibling)

    sums = exchange_x(projection(where, hidden, extra, [moved[d] for d in (1, 2, 3)], four, rest))
    vis = jnp.sum(sums[:, tokens:], axis=0).astype(jnp.bfloat16).reshape(NS, CAP, cols)
    marks = jnp.broadcast_to(vis_slot.reshape(NS, CAP, 1), (NS, CAP, tokens)).astype(jnp.bfloat16)
    vis = lax.all_to_all(jnp.concatenate([vis, marks], axis=2), "seq", 0, 0, tiled=True)
    docs = jnp.broadcast_to(jnp.tile(doc_ids, (1, cols // tokens)), (8, cols)).astype(jnp.bfloat16)
    block = merged_block(sums[:, :tokens], vis.reshape(NS * CAP, -1), docs)

    back = [seq_permute(block, later(d)) for d in range(1, REACH + 1)]
    mine = jnp.stack([block, *back])
    other = seq_permute(mine, sibling)
    my_docs = doc_ids.reshape(tokens, 1).astype(jnp.float32)
    return attention(where, queries, mine, other, my_docs)


def solution(mesh):
    return jax.shard_map(
        program,
        mesh=mesh,
        in_specs=(
            P(("grp", "seq"), None),
            P(("grp", "seq"), "tp"),
            P(("grp", "seq"), None, None, None),
            P(("grp", "seq"), None, None),
            P("grp", "seq"),
            P("grp", "tp"),
            P("grp", "tp"),
        ),
        out_specs=P(("grp", "seq"), "tp"),
        check_vma=False,
    )
```

```python
import jax
import jax.numpy as jnp
from jax import lax
from jax.experimental import pallas as pl
from jax.experimental.pallas import tpu as pltpu
from jax.sharding import PartitionSpec as P


HEAD = 128
QPK = 8
CAP = 4
HEADS_STEP = 4
NX = 4
NZ = 4
NLO = 8
NS = 16
NT = 4
REACH = 4
AXES = ("grp", "seq", "tp")
OVER_X = [[x * NZ + z for x in range(NX)] for z in range(NZ)]
OVER_X_SEQ = [[(x * NZ + z) * NS + s for x in range(NX) for s in range(NS)] for z in range(NZ)]
OVER_Z = [[x * NZ + z for z in range(NZ)] for x in range(NX)]


def seq_permute(array, move):
    pairs = []
    for g in range(NX * NZ):
        for s in range(NS):
            to = move(s // 2, s % 2)
            if to is None:
                continue
            for t in range(NT):
                pairs.append(((g * NS + s) * NT + t, (g * NS + to[0] * 2 + to[1]) * NT + t))
    return lax.ppermute(array, AXES, pairs)


def x_permute(array, d):
    step, size = NZ * NS * NT, NX * NZ * NS * NT
    return lax.ppermute(array, AXES, [(i, (i + d * step) % size) for i in range(size)])


def sibling(z, c):
    return z, 1 - c


def flip(mask):
    return lambda z, c: (z ^ mask, c)


def later(d):
    return lambda z, c: (z + d, c) if z + d < NLO else None


MIB = 1 << 20
IN_VMEM = pl.BlockSpec(memory_space=pltpu.VMEM)


def in_vmem(array):
    return pltpu.with_memory_space_constraint(array, pltpu.VMEM)


def in_hbm(array):
    return pltpu.with_memory_space_constraint(array, pltpu.HBM)


def pack(text_ref, extra_ref, out_ref):
    tokens = text_ref.shape[0]
    out_ref[0, :tokens, :] = text_ref[...]
    out_ref[0, tokens:, :] = extra_ref[0].reshape(NS * CAP, -1)


def packed(hidden, vis_rows):
    tokens, width = hidden.shape
    count = tokens + NS * CAP
    part = width // NX
    return pl.pallas_call(
        pack,
        grid=(NX,),
        in_specs=[
            pl.BlockSpec((tokens, part), lambda i: (0, i)),
            pl.BlockSpec((1, NS, CAP, part), lambda i: (0, 0, 0, i)),
        ],
        out_specs=pl.BlockSpec((1, count, part), lambda i: (i, 0, 0)),
        out_shape=pltpu.HBM((NX, count, part), hidden.dtype),
        compiler_params=pltpu.CompilerParams(vmem_limit_bytes=16 * MIB),
        name="pack",
    )(in_hbm(hidden), in_hbm(vis_rows))


def project(place_ref, rows_ref, mine_ref, other_ref, marks_ref, vis_ref, *refs):
    *text_refs, weights_ref = refs
    steps, sources, part, cols = mine_ref.shape
    tokens = text_refs[0].shape[0]
    s, x = place_ref[0], place_ref[1]
    core, chip = lax.rem(s, 2), lax.rem(s // 2, 4)
    for side, ref in enumerate((mine_ref, other_ref)):
        at = pl.ds(pl.multiple_of(jnp.where(core == side, 0, cols), cols), cols)
        for k in range(steps):
            piece = 2 * lax.rem(chip // 2 + k % 2, 2) + lax.rem(chip + k // 2, 2)
            for z in range(sources):
                row = pl.ds(pl.multiple_of(z * steps * part + piece * part, part), part)
                weights_ref[row, at] = ref[k, z]
    weights = weights_ref[...]
    marks = marks_ref[...]
    for block in range(NX):
        vis = jnp.dot(rows_ref[block, tokens:, :], weights, preferred_element_type=jnp.float32)
        slots = jnp.where(x == block, marks, jnp.zeros_like(marks))
        for i in range(NS):
            vis_ref[block * NS + i, :, : 2 * cols] = vis[i * CAP : (i + 1) * CAP]
            vis_ref[block * NS + i, :, 2 * cols :] = slots[i * CAP : (i + 1) * CAP]
    for d, ref in enumerate(text_refs):
        ref[...] = jnp.dot(
            rows_ref[lax.rem(x + d, NX), :tokens, :], weights, preferred_element_type=jnp.float32
        )


def projection(place, rows, mine, other, marks):
    blocks, count, part = rows.shape
    cols = 2 * mine.shape[-1]
    extra = NS * CAP
    text = pltpu.VMEM((count - extra, cols), jnp.float32)
    vis = jax.ShapeDtypeStruct((blocks * NS, CAP, cols + marks.shape[1]), jnp.float32)
    return pl.pallas_call(
        project,
        grid_spec=pltpu.PrefetchScalarGridSpec(
            num_scalar_prefetch=1,
            grid=(1,),
            in_specs=[IN_VMEM] * 4,
            out_specs=[pl.BlockSpec(vis.shape, lambda i, _: (0, 0, 0))] + [IN_VMEM] * blocks,
            scratch_shapes=[pltpu.VMEM((part, cols), jnp.bfloat16)],
        ),
        out_shape=[vis] + [text] * blocks,
        compiler_params=pltpu.CompilerParams(vmem_limit_bytes=16 * MIB),
        name="project",
    )(place, *map(in_vmem, (rows, mine, other)), marks)


def merge(vis_ref, docs_ref, *refs):
    *text_refs, out_ref = refs
    tokens, cols = text_refs[0].shape
    text = (text_refs[0][...] + text_refs[1][...]) + (text_refs[2][...] + text_refs[3][...])
    vis = vis_ref[...]
    vis = (vis[:NS] + vis[NS : 2 * NS]) + (vis[2 * NS : 3 * NS] + vis[3 * NS :])
    vis = vis.reshape(NS * CAP, vis.shape[-1])
    slots = vis[:, cols:]
    matches = slots == lax.broadcasted_iota(jnp.int32, slots.shape, 1).astype(jnp.float32)
    chooser = matches.astype(jnp.float32).astype(jnp.bfloat16)
    dims = (((0,), (0,)), ((), ()))
    moved = lax.dot_general(
        chooser, vis[:, :cols].astype(jnp.bfloat16), dims, preferred_element_type=jnp.float32
    )
    ones = jnp.ones((slots.shape[0], cols), jnp.bfloat16)
    used = lax.dot_general(chooser, ones, dims, preferred_element_type=jnp.float32)
    out_ref[:tokens, :] = jnp.where(used > 0.5, moved, text).astype(jnp.bfloat16)
    out_ref[tokens:, :] = docs_ref[...]


def merged_block(vis, docs, text):
    tokens, cols = text[0].shape
    return pl.pallas_call(
        merge,
        in_specs=[IN_VMEM] * (2 + len(text)),
        out_specs=IN_VMEM,
        out_shape=pltpu.VMEM((tokens + docs.shape[0], cols), jnp.bfloat16),
        compiler_params=pltpu.CompilerParams(vmem_limit_bytes=8 * MIB),
        name="merge",
    )(in_vmem(vis), docs, *map(in_vmem, text))


def attend(place_ref, q_ref, mine_ref, other_ref, my_docs_ref, out_ref, bias_ref, keys_ref, values_ref):
    tokens = q_ref.shape[0]
    blocks = mine_ref.shape[0]

    @pl.when(pl.program_id(0) == 0)
    def _():
        s = place_ref[0]
        core, chip = lax.rem(s, 2), s // 2
        my_docs = jnp.broadcast_to(my_docs_ref[...], (tokens, tokens))
        row = lax.broadcasted_iota(jnp.int32, (tokens, tokens), 0) + s * tokens
        col = lax.broadcasted_iota(jnp.int32, (tokens, tokens), 1)
        for side, ref in enumerate((mine_ref, other_ref)):
            for d in range(blocks):
                block = 2 * (chip - d) + (core if side == 0 else 1 - core)
                docs = ref[d, tokens : tokens + 8, :tokens].astype(jnp.float32)[:1]
                spot = col + block * tokens
                allowed = (docs == my_docs) & (spot <= row) & (spot >= 0)
                at = (side * blocks + d) * tokens
                bias_ref[:, at : at + tokens] = jnp.where(allowed, 0.0, -1e30)
                keys_ref[at : at + tokens, :] = ref[d, :tokens, :HEAD]
                values_ref[at : at + tokens, :] = ref[d, :tokens, HEAD:]

    scale = 1.0 / jnp.sqrt(jnp.float32(HEAD))
    for h in range(HEADS_STEP):
        head = slice(h * HEAD, (h + 1) * HEAD)
        scores = lax.dot_general(
            q_ref[:, head], keys_ref[...], (((1,), (1,)), ((), ())), preferred_element_type=jnp.float32
        )
        scores = scores * scale + bias_ref[...]
        top = jnp.max(scores, axis=1, keepdims=True)
        weights = jnp.exp(scores - top)
        total = jnp.sum(weights, axis=1, keepdims=True)
        mixed = jnp.dot(
            weights.astype(jnp.bfloat16), values_ref[...], preferred_element_type=jnp.float32
        )
        out_ref[:, head] = (mixed / total).astype(out_ref.dtype)


def attention(place, queries, mine, other, my_docs):
    tokens = queries.shape[0]
    span = 2 * mine.shape[0] * tokens
    return pl.pallas_call(
        attend,
        grid_spec=pltpu.PrefetchScalarGridSpec(
            num_scalar_prefetch=1,
            grid=(QPK // HEADS_STEP,),
            in_specs=[
                pl.BlockSpec((tokens, HEADS_STEP * HEAD), lambda h, *_: (0, h)),
                IN_VMEM,
                IN_VMEM,
                IN_VMEM,
            ],
            out_specs=pl.BlockSpec((tokens, HEADS_STEP * HEAD), lambda h, *_: (0, h)),
            scratch_shapes=[
                pltpu.VMEM((tokens, span), jnp.float32),
                pltpu.VMEM((span, HEAD), jnp.bfloat16),
                pltpu.VMEM((span, HEAD), jnp.bfloat16),
            ],
        ),
        out_shape=jax.ShapeDtypeStruct(queries.shape, jnp.bfloat16),
        compiler_params=pltpu.CompilerParams(vmem_limit_bytes=16 * MIB),
        name="attend",
    )(place, queries, in_vmem(mine), in_vmem(other), my_docs)


def exchange_x(array):
    return lax.all_to_all(array, "grp", 0, 0, axis_index_groups=OVER_X, tiled=True)


def program(hidden, queries, vis_rows, vis_slot, doc_ids, w_key, w_value):
    tokens = hidden.shape[0]
    cols = 2 * w_key.shape[1]
    place = lax.axis_index("seq")
    core, chip = place % 2, place // 2
    x = lax.axis_index("grp") // NZ
    where = jnp.stack([place, x])

    part = w_key.shape[0] // 4
    start = (chip % 4) * part
    piece = jnp.where(
        core == 0,
        lax.dynamic_slice_in_dim(w_key, start, part, axis=0),
        lax.dynamic_slice_in_dim(w_value, start, part, axis=0),
    )
    got = lax.all_gather(piece, "grp", axis=0, axis_index_groups=OVER_Z)

    rows = exchange_x(packed(hidden, vis_rows))

    far = seq_permute(got, flip(2))
    pair = jnp.stack([got, far])
    near = seq_permute(pair, flip(1))
    four = jnp.concatenate([pair, near])
    rest = seq_permute(four, sibling)

    marks = jnp.broadcast_to(vis_slot.reshape(NS * CAP, 1), (NS * CAP, tokens)).astype(jnp.float32)
    vis, *text = projection(where, rows, four, rest, marks)
    vis = lax.all_to_all(
        vis, ("grp", "seq"), 0, 0, axis_index_groups=OVER_X_SEQ, tiled=True
    )
    for d in (2, 1, 3):
        text[d] = x_permute(in_vmem(text[d]), d)
    docs = jnp.broadcast_to(jnp.tile(doc_ids, (1, cols // tokens)), (8, cols)).astype(jnp.bfloat16)
    block = merged_block(vis, docs, text)

    back = [seq_permute(block, later(d)) for d in range(1, REACH + 1)]
    mine = jnp.stack([block, *back])
    other = seq_permute(mine, sibling)
    my_docs = doc_ids.reshape(tokens, 1).astype(jnp.float32)
    return attention(where, queries, mine, other, my_docs)


def solution(mesh):
    return jax.shard_map(
        program,
        mesh=mesh,
        in_specs=(
            P(("grp", "seq"), None),
            P(("grp", "seq"), "tp"),
            P(("grp", "seq"), None, None, None),
            P(("grp", "seq"), None, None),
            P("grp", "seq"),
            P("grp", "tp"),
            P("grp", "tp"),
        ),
        out_specs=P(("grp", "seq"), "tp"),
        check_vma=False,
    )
```

```python
import jax
import jax.numpy as jnp
from jax import lax
from jax.experimental import pallas as pl
from jax.experimental.pallas import tpu as pltpu
from jax.sharding import PartitionSpec as P


HEAD = 128
QPK = 8
CAP = 4
HEADS_STEP = 4
NX = 4
NZ = 4
NLO = 8
NS = 16
NT = 4
REACH = 4
AXES = ("grp", "seq", "tp")
OVER_X = [[x * NZ + z for x in range(NX)] for z in range(NZ)]
OVER_Z = [[x * NZ + z for z in range(NZ)] for x in range(NX)]
NEAR = 4
OVER_NEAR = [
    [(first + i) * 2 + core for i in range(NEAR)] for first in range(0, NLO, NEAR) for core in range(2)
]


def seq_permute(array, move):
    pairs = []
    for g in range(NX * NZ):
        for s in range(NS):
            to = move(s // 2, s % 2)
            if to is None:
                continue
            for t in range(NT):
                pairs.append(((g * NS + s) * NT + t, (g * NS + to[0] * 2 + to[1]) * NT + t))
    return lax.ppermute(array, AXES, pairs)


def x_permute(array, d):
    step, size = NZ * NS * NT, NX * NZ * NS * NT
    return lax.ppermute(array, AXES, [(i, (i + d * step) % size) for i in range(size)])


def sibling(z, c):
    return z, 1 - c


def later(d):
    return lambda z, c: (z + d, c) if z + d < NLO else None


MIB = 1 << 20
IN_VMEM = pl.BlockSpec(memory_space=pltpu.VMEM)


def in_vmem(array):
    return pltpu.with_memory_space_constraint(array, pltpu.VMEM)


def in_hbm(array):
    return pltpu.with_memory_space_constraint(array, pltpu.HBM)


def pack(text_ref, extra_ref, out_ref):
    tokens = text_ref.shape[0]
    out_ref[0, :tokens, :] = text_ref[...]
    out_ref[0, tokens:, :] = extra_ref[0].reshape(NS * CAP, -1)


def packed(hidden, vis_rows):
    tokens, width = hidden.shape
    count = tokens + NS * CAP
    part = width // NX
    return pl.pallas_call(
        pack,
        grid=(NX,),
        in_specs=[
            pl.BlockSpec((tokens, part), lambda i: (0, i)),
            pl.BlockSpec((1, NS, CAP, part), lambda i: (0, 0, 0, i)),
        ],
        out_specs=pl.BlockSpec((1, count, part), lambda i: (i, 0, 0)),
        out_shape=pltpu.HBM((NX, count, part), hidden.dtype),
        compiler_params=pltpu.CompilerParams(vmem_limit_bytes=16 * MIB),
        name="pack",
    )(in_hbm(hidden), in_hbm(vis_rows))


def project_extra(place_ref, rows_ref, mine_ref, other_ref, vis_ref, weights_ref):
    steps, sources, part, cols = mine_ref.shape
    tokens = rows_ref.shape[1] - NS * CAP
    core = lax.rem(place_ref[0], 2)
    for side, ref in enumerate((mine_ref, other_ref)):
        at = pl.ds(pl.multiple_of(jnp.where(core == side, 0, cols), cols), cols)
        for k in range(steps):
            for z in range(sources):
                row = (z * steps + k) * part
                weights_ref[row : row + part, at] = ref[k, z]
    weights = weights_ref[...]
    for block in range(NX):
        vis_ref[block] = jnp.dot(
            rows_ref[block, tokens:, :], weights, preferred_element_type=jnp.float32
        )


def projected_extra(place, rows, mine, other):
    blocks, _, part = rows.shape
    cols = 2 * mine.shape[-1]
    vis = pltpu.HBM((blocks, NS * CAP, cols), jnp.float32)
    return pl.pallas_call(
        project_extra,
        grid_spec=pltpu.PrefetchScalarGridSpec(
            num_scalar_prefetch=1,
            grid=(1,),
            in_specs=[IN_VMEM] * 3,
            out_specs=[pl.BlockSpec(vis.shape, lambda i, _: (0, 0, 0)), IN_VMEM],
        ),
        out_shape=[vis, pltpu.VMEM((part, cols), jnp.bfloat16)],
        compiler_params=pltpu.CompilerParams(vmem_limit_bytes=16 * MIB),
        name="project_extra",
    )(place, *map(in_vmem, (rows, mine, other)))


def project_text(place_ref, rows_ref, weights_ref, own_ref, *text_refs):
    tokens = own_ref.shape[0]
    x = place_ref[1]
    for d, ref in enumerate((own_ref, *text_refs)):
        ref[...] = jnp.dot(
            rows_ref[lax.rem(x + d, NX), :tokens, :],
            weights_ref[...],
            preferred_element_type=jnp.float32,
        )


def projected_text(place, rows, weights):
    blocks, count, _ = rows.shape
    shape = (count - NS * CAP, weights.shape[1])
    return pl.pallas_call(
        project_text,
        grid_spec=pltpu.PrefetchScalarGridSpec(
            num_scalar_prefetch=1,
            grid=(1,),
            in_specs=[IN_VMEM] * 2,
            out_specs=[IN_VMEM] + [pl.BlockSpec(shape, lambda i, _: (0, 0))] * (blocks - 1),
        ),
        out_shape=[pltpu.VMEM(shape, jnp.float32)]
        + [pltpu.HBM(shape, jnp.float32)] * (blocks - 1),
        compiler_params=pltpu.CompilerParams(vmem_limit_bytes=16 * MIB),
        name="project_text",
    )(place, *map(in_vmem, (rows, weights)))


def settle(sums_ref, marks_ref, out_ref):
    cols = sums_ref.shape[-1]
    rows = (sums_ref[0] + sums_ref[1]) + (sums_ref[2] + sums_ref[3])
    for i in range(NS):
        at = slice(i * CAP, (i + 1) * CAP)
        out_ref[i, :, :cols] = rows[at].astype(jnp.bfloat16)
        out_ref[i, :, cols:] = marks_ref[at, :].astype(jnp.bfloat16)


def settled(sums, marks):
    shape = (NS, CAP, sums.shape[-1] + marks.shape[-1])
    return pl.pallas_call(
        settle,
        grid=(1,),
        in_specs=[IN_VMEM] * 2,
        out_specs=pl.BlockSpec(shape, lambda i: (0, 0, 0)),
        out_shape=pltpu.HBM(shape, jnp.bfloat16),
        compiler_params=pltpu.CompilerParams(vmem_limit_bytes=8 * MIB),
        name="settle",
    )(in_vmem(sums), marks)


def merge(vis_ref, docs_ref, *refs):
    *text_refs, out_ref = refs
    tokens, cols = text_refs[0].shape
    text = (text_refs[0][...] + text_refs[1][...]) + (text_refs[2][...] + text_refs[3][...])
    vis = vis_ref[...].reshape(NS * CAP, vis_ref.shape[-1])
    slots = vis[:, cols:].astype(jnp.float32)
    matches = slots == lax.broadcasted_iota(jnp.int32, slots.shape, 1).astype(jnp.float32)
    chooser = matches.astype(jnp.float32).astype(jnp.bfloat16)
    dims = (((0,), (0,)), ((), ()))
    moved = lax.dot_general(chooser, vis[:, :cols], dims, preferred_element_type=jnp.float32)
    ones = jnp.ones((slots.shape[0], cols), jnp.bfloat16)
    used = lax.dot_general(chooser, ones, dims, preferred_element_type=jnp.float32)
    out_ref[:tokens, :] = jnp.where(used > 0.5, moved, text).astype(jnp.bfloat16)
    out_ref[tokens:, :] = docs_ref[...]


def merged_block(vis, docs, text):
    tokens, cols = text[0].shape
    return pl.pallas_call(
        merge,
        in_specs=[IN_VMEM] * (2 + len(text)),
        out_specs=IN_VMEM,
        out_shape=pltpu.VMEM((tokens + docs.shape[0], cols), jnp.bfloat16),
        compiler_params=pltpu.CompilerParams(vmem_limit_bytes=8 * MIB),
        name="merge",
    )(in_vmem(vis), docs, *map(in_vmem, text))


def attend(place_ref, q_ref, mine_ref, other_ref, my_docs_ref, out_ref, bias_ref, keys_ref, values_ref):
    tokens = q_ref.shape[0]
    blocks = mine_ref.shape[0]

    @pl.when(pl.program_id(0) == 0)
    def _():
        s = place_ref[0]
        core, chip = lax.rem(s, 2), s // 2
        my_docs = jnp.broadcast_to(my_docs_ref[...], (tokens, tokens))
        row = lax.broadcasted_iota(jnp.int32, (tokens, tokens), 0) + s * tokens
        col = lax.broadcasted_iota(jnp.int32, (tokens, tokens), 1)
        for side, ref in enumerate((mine_ref, other_ref)):
            for d in range(blocks):
                block = 2 * (chip - d) + (core if side == 0 else 1 - core)
                docs = ref[d, tokens : tokens + 8, :tokens].astype(jnp.float32)[:1]
                spot = col + block * tokens
                allowed = (docs == my_docs) & (spot <= row) & (spot >= 0)
                at = (side * blocks + d) * tokens
                bias_ref[:, at : at + tokens] = jnp.where(allowed, 0.0, -1e30)
                keys_ref[at : at + tokens, :] = ref[d, :tokens, :HEAD]
                values_ref[at : at + tokens, :] = ref[d, :tokens, HEAD:]

    scale = 1.0 / jnp.sqrt(jnp.float32(HEAD))
    for h in range(HEADS_STEP):
        head = slice(h * HEAD, (h + 1) * HEAD)
        scores = lax.dot_general(
            q_ref[:, head], keys_ref[...], (((1,), (1,)), ((), ())), preferred_element_type=jnp.float32
        )
        scores = scores * scale + bias_ref[...]
        top = jnp.max(scores, axis=1, keepdims=True)
        weights = jnp.exp(scores - top)
        total = jnp.sum(weights, axis=1, keepdims=True)
        mixed = jnp.dot(
            weights.astype(jnp.bfloat16), values_ref[...], preferred_element_type=jnp.float32
        )
        out_ref[:, head] = (mixed / total).astype(out_ref.dtype)


def attention(place, queries, mine, other, my_docs):
    tokens = queries.shape[0]
    span = 2 * mine.shape[0] * tokens
    return pl.pallas_call(
        attend,
        grid_spec=pltpu.PrefetchScalarGridSpec(
            num_scalar_prefetch=1,
            grid=(QPK // HEADS_STEP,),
            in_specs=[
                pl.BlockSpec((tokens, HEADS_STEP * HEAD), lambda h, *_: (0, h)),
                IN_VMEM,
                IN_VMEM,
                IN_VMEM,
            ],
            out_specs=pl.BlockSpec((tokens, HEADS_STEP * HEAD), lambda h, *_: (0, h)),
            scratch_shapes=[
                pltpu.VMEM((tokens, span), jnp.float32),
                pltpu.VMEM((span, HEAD), jnp.bfloat16),
                pltpu.VMEM((span, HEAD), jnp.bfloat16),
            ],
        ),
        out_shape=jax.ShapeDtypeStruct(queries.shape, jnp.bfloat16),
        compiler_params=pltpu.CompilerParams(vmem_limit_bytes=16 * MIB),
        name="attend",
    )(place, queries, in_vmem(mine), in_vmem(other), my_docs)


def exchange_x(array):
    return lax.all_to_all(array, "grp", 0, 0, axis_index_groups=OVER_X, tiled=True)


def program(hidden, queries, vis_rows, vis_slot, doc_ids, w_key, w_value):
    tokens = hidden.shape[0]
    cols = 2 * w_key.shape[1]
    place = lax.axis_index("seq")
    core, chip = place % 2, place // 2
    x = lax.axis_index("grp") // NZ
    where = jnp.stack([place, x])

    part = w_key.shape[0] // NEAR
    start = (chip % NEAR) * part
    piece = jnp.where(
        core == 0,
        lax.dynamic_slice_in_dim(w_key, start, part, axis=0),
        lax.dynamic_slice_in_dim(w_value, start, part, axis=0),
    )
    got = lax.all_gather(piece, "grp", axis=0, axis_index_groups=OVER_Z)

    rows = exchange_x(packed(hidden, vis_rows))

    mine = lax.all_gather(got, "seq", axis=0, axis_index_groups=OVER_NEAR)
    other = seq_permute(mine, sibling)

    vis, weights = projected_extra(where, rows, mine, other)
    vis = exchange_x(vis)
    text = list(projected_text(where, rows, weights))
    for d in (2, 1, 3):
        text[d] = x_permute(text[d], d)
    marks = jnp.broadcast_to(vis_slot.reshape(NS * CAP, 1), (NS * CAP, tokens)).astype(jnp.float32)
    vis = settled(vis, marks)
    vis = lax.all_to_all(vis, "seq", 0, 0, tiled=True)
    docs = jnp.broadcast_to(jnp.tile(doc_ids, (1, cols // tokens)), (8, cols)).astype(jnp.bfloat16)
    block = merged_block(vis, docs, text)

    back = [seq_permute(block, later(d)) for d in range(1, REACH + 1)]
    mine = jnp.stack([block, *back])
    other = seq_permute(mine, sibling)
    my_docs = doc_ids.reshape(tokens, 1).astype(jnp.float32)
    return attention(where, queries, mine, other, my_docs)


def solution(mesh):
    return jax.shard_map(
        program,
        mesh=mesh,
        in_specs=(
            P(("grp", "seq"), None),
            P(("grp", "seq"), "tp"),
            P(("grp", "seq"), None, None, None),
            P(("grp", "seq"), None, None),
            P("grp", "seq"),
            P("grp", "tp"),
            P("grp", "tp"),
        ),
        out_specs=P(("grp", "seq"), "tp"),
        check_vma=False,
    )
```

```python
import jax
import jax.numpy as jnp
from jax import lax
from jax.experimental import pallas as pl
from jax.experimental.pallas import tpu as pltpu
from jax.sharding import PartitionSpec as P


HEAD = 128
QPK = 8
CAP = 4
HEADS_STEP = 4
NX = 4
NZ = 4
NLO = 8
NS = 16
NT = 4
REACH = 4
AXES = ("grp", "seq", "tp")
OVER_X = [[x * NZ + z for x in range(NX)] for z in range(NZ)]
OVER_Z = [[x * NZ + z for z in range(NZ)] for x in range(NX)]
NEAR = 4
OVER_NEAR = [
    [(first + i) * 2 + core for i in range(NEAR)] for first in range(0, NLO, NEAR) for core in range(2)
]


def seq_permute(array, move):
    pairs = []
    for g in range(NX * NZ):
        for s in range(NS):
            to = move(s // 2, s % 2)
            if to is None:
                continue
            for t in range(NT):
                pairs.append(((g * NS + s) * NT + t, (g * NS + to[0] * 2 + to[1]) * NT + t))
    return lax.ppermute(array, AXES, pairs)


def x_permute(array, d):
    step, size = NZ * NS * NT, NX * NZ * NS * NT
    return lax.ppermute(array, AXES, [(i, (i + d * step) % size) for i in range(size)])


def sibling(z, c):
    return z, 1 - c


def later(d):
    return lambda z, c: (z + d, c) if z + d < NLO else None


MIB = 1 << 20
IN_VMEM = pl.BlockSpec(memory_space=pltpu.VMEM)


def whole(shape):
    return pl.BlockSpec(shape, lambda *_: (0,) * len(shape))


def in_vmem(array):
    return pltpu.with_memory_space_constraint(array, pltpu.VMEM)


def in_hbm(array):
    return pltpu.with_memory_space_constraint(array, pltpu.HBM)


def pack(place_ref, text_ref, extra_ref, key_ref, value_ref, out_ref, piece_ref, *scratch):
    extra_in, extra_out, key_part, value_part, text_sem, in_sem, out_sem, piece_sem = scratch
    tokens = text_ref.shape[0]
    width = out_ref.shape[2]
    part = piece_ref.shape[0]
    s = place_ref[0]
    rows = pl.ds(pl.multiple_of(lax.rem(s // 2, NEAR) * part, part), part)
    pieces = [
        pltpu.make_async_copy(key_ref.at[rows], key_part, piece_sem.at[0]),
        pltpu.make_async_copy(value_ref.at[rows], value_part, piece_sem.at[1]),
    ]
    texts, ins, outs = [], [], []
    for q in range(NX):
        cols = pl.ds(q * width, width)
        ins.append(pltpu.make_async_copy(extra_ref.at[0, :, :, cols], extra_in.at[q], in_sem.at[q]))
        texts.append(
            pltpu.make_async_copy(
                text_ref.at[:, cols], out_ref.at[q, pl.ds(0, tokens)], text_sem.at[q]
            )
        )
        outs.append(
            pltpu.make_async_copy(
                extra_out.at[q], out_ref.at[q, pl.ds(tokens, NS * CAP)], out_sem.at[q]
            )
        )
    for copy in (*ins, *texts, *pieces):
        copy.start()
    for q in range(NX):
        ins[q].wait()
        extra_out[q] = extra_in[q].reshape(NS * CAP, width)
        outs[q].start()
    for copy in pieces:
        copy.wait()
    piece_ref[...] = jnp.where(lax.rem(s, 2) == 0, key_part[...], value_part[...])
    for copy in (*texts, *outs):
        copy.wait()


def packed(place, hidden, vis_rows, w_key, w_value):
    tokens, width = hidden.shape
    extra = NS * CAP
    part = width // NX
    piece = (w_key.shape[0] // NEAR, w_key.shape[1])
    kind = hidden.dtype
    anywhere = pl.BlockSpec(memory_space=pl.ANY)
    return pl.pallas_call(
        pack,
        grid_spec=pltpu.PrefetchScalarGridSpec(
            num_scalar_prefetch=1,
            grid=(1,),
            in_specs=[anywhere] * 4,
            out_specs=[anywhere, IN_VMEM],
            scratch_shapes=[
                pltpu.VMEM((NX, NS, CAP, part), kind),
                pltpu.VMEM((NX, extra, part), kind),
                pltpu.VMEM(piece, kind),
                pltpu.VMEM(piece, kind),
                pltpu.SemaphoreType.DMA((NX,)),
                pltpu.SemaphoreType.DMA((NX,)),
                pltpu.SemaphoreType.DMA((NX,)),
                pltpu.SemaphoreType.DMA((2,)),
            ],
        ),
        out_shape=[pltpu.HBM((NX, tokens + extra, part), kind), pltpu.VMEM(piece, kind)],
        compiler_params=pltpu.CompilerParams(vmem_limit_bytes=16 * MIB),
        name="pack",
    )(place, *map(in_hbm, (hidden, vis_rows, w_key, w_value)))


def order(place_ref, mine_ref, other_ref, weights_ref):
    steps, sources, part, cols = mine_ref.shape
    core = lax.rem(place_ref[0], 2)
    for side, ref in enumerate((mine_ref, other_ref)):
        at = pl.ds(pl.multiple_of(jnp.where(core == side, 0, cols), cols), cols)
        for k in range(steps):
            for z in range(sources):
                row = (z * steps + k) * part
                weights_ref[row : row + part, at] = ref[k, z]


def project_extra(place_ref, rows_ref, mine_ref, other_ref, vis_ref, weights_ref):
    tokens = rows_ref.shape[1] - NS * CAP
    order(place_ref, mine_ref, other_ref, weights_ref)
    weights = weights_ref[...]
    for block in range(NX):
        vis_ref[block] = jnp.dot(
            rows_ref[block, tokens:, :], weights, preferred_element_type=jnp.float32
        )


def projected_extra(place, rows, mine, other):
    blocks, _, part = rows.shape
    cols = 2 * mine.shape[-1]
    vis = pltpu.HBM((blocks, NS * CAP, cols), jnp.float32)
    return pl.pallas_call(
        project_extra,
        grid_spec=pltpu.PrefetchScalarGridSpec(
            num_scalar_prefetch=1,
            grid=(1,),
            in_specs=[IN_VMEM, whole(mine.shape), whole(other.shape)],
            out_specs=pl.BlockSpec(vis.shape, lambda i, _: (0, 0, 0)),
            scratch_shapes=[pltpu.VMEM((part, cols), jnp.bfloat16)],
        ),
        out_shape=vis,
        compiler_params=pltpu.CompilerParams(vmem_limit_bytes=16 * MIB),
        name="project_extra",
    )(place, in_vmem(rows), in_hbm(mine), in_hbm(other))


def project_text(place_ref, rows_ref, mine_ref, other_ref, own_ref, *refs):
    *text_refs, weights_ref = refs
    tokens = own_ref.shape[0]
    x = place_ref[1]
    order(place_ref, mine_ref, other_ref, weights_ref)
    weights = weights_ref[...]
    for d, ref in enumerate((own_ref, *text_refs)):
        ref[...] = jnp.dot(
            rows_ref[lax.rem(x + d, NX), :tokens, :], weights, preferred_element_type=jnp.float32
        )


def projected_text(place, rows, mine, other):
    blocks, count, part = rows.shape
    shape = (count - NS * CAP, 2 * mine.shape[-1])
    return pl.pallas_call(
        project_text,
        grid_spec=pltpu.PrefetchScalarGridSpec(
            num_scalar_prefetch=1,
            grid=(1,),
            in_specs=[IN_VMEM, whole(mine.shape), whole(other.shape)],
            out_specs=[IN_VMEM] + [pl.BlockSpec(shape, lambda i, _: (0, 0))] * (blocks - 1),
            scratch_shapes=[pltpu.VMEM((part, shape[1]), jnp.bfloat16)],
        ),
        out_shape=[pltpu.VMEM(shape, jnp.float32)]
        + [pltpu.HBM(shape, jnp.float32)] * (blocks - 1),
        compiler_params=pltpu.CompilerParams(vmem_limit_bytes=16 * MIB),
        name="project_text",
    )(place, in_vmem(rows), in_hbm(mine), in_hbm(other))


def settle(sums_ref, marks_ref, out_ref):
    cols = sums_ref.shape[-1]
    rows = (sums_ref[0] + sums_ref[1]) + (sums_ref[2] + sums_ref[3])
    for i in range(NS):
        at = slice(i * CAP, (i + 1) * CAP)
        out_ref[i, :, :cols] = rows[at].astype(jnp.bfloat16)
        out_ref[i, :, cols:] = marks_ref[at, :].astype(jnp.bfloat16)


def settled(sums, marks):
    shape = (NS, CAP, sums.shape[-1] + marks.shape[-1])
    return pl.pallas_call(
        settle,
        grid=(1,),
        in_specs=[IN_VMEM] * 2,
        out_specs=pl.BlockSpec(shape, lambda i: (0, 0, 0)),
        out_shape=pltpu.HBM(shape, jnp.bfloat16),
        compiler_params=pltpu.CompilerParams(vmem_limit_bytes=8 * MIB),
        name="settle",
    )(in_vmem(sums), marks)


def merge(vis_ref, docs_ref, *refs):
    *text_refs, out_ref = refs
    tokens, cols = text_refs[0].shape
    text = (text_refs[0][...] + text_refs[1][...]) + (text_refs[2][...] + text_refs[3][...])
    vis = vis_ref[...].reshape(NS * CAP, vis_ref.shape[-1])
    slots = vis[:, cols:].astype(jnp.float32)
    matches = slots == lax.broadcasted_iota(jnp.int32, slots.shape, 1).astype(jnp.float32)
    chooser = matches.astype(jnp.float32).astype(jnp.bfloat16)
    dims = (((0,), (0,)), ((), ()))
    moved = lax.dot_general(chooser, vis[:, :cols], dims, preferred_element_type=jnp.float32)
    ones = jnp.ones((slots.shape[0], cols), jnp.bfloat16)
    used = lax.dot_general(chooser, ones, dims, preferred_element_type=jnp.float32)
    out_ref[:tokens, :] = jnp.where(used > 0.5, moved, text).astype(jnp.bfloat16)
    out_ref[tokens:, :] = docs_ref[...]


def merged_block(vis, docs, text):
    tokens, cols = text[0].shape
    return pl.pallas_call(
        merge,
        in_specs=[IN_VMEM] * (2 + len(text)),
        out_specs=IN_VMEM,
        out_shape=pltpu.VMEM((tokens + docs.shape[0], cols), jnp.bfloat16),
        compiler_params=pltpu.CompilerParams(vmem_limit_bytes=8 * MIB),
        name="merge",
    )(in_vmem(vis), docs, *map(in_vmem, text))


def attend(place_ref, q_ref, mine_ref, other_ref, my_docs_ref, out_ref, bias_ref, keys_ref, values_ref):
    tokens = q_ref.shape[0]
    blocks = mine_ref.shape[0]

    @pl.when(pl.program_id(0) == 0)
    def _():
        s = place_ref[0]
        core, chip = lax.rem(s, 2), s // 2
        my_docs = jnp.broadcast_to(my_docs_ref[...], (tokens, tokens))
        row = lax.broadcasted_iota(jnp.int32, (tokens, tokens), 0) + s * tokens
        col = lax.broadcasted_iota(jnp.int32, (tokens, tokens), 1)
        for side, ref in enumerate((mine_ref, other_ref)):
            for d in range(blocks):
                block = 2 * (chip - d) + (core if side == 0 else 1 - core)
                docs = ref[d, tokens : tokens + 8, :tokens].astype(jnp.float32)[:1]
                spot = col + block * tokens
                allowed = (docs == my_docs) & (spot <= row) & (spot >= 0)
                at = (side * blocks + d) * tokens
                bias_ref[:, at : at + tokens] = jnp.where(allowed, 0.0, -1e30)
                keys_ref[at : at + tokens, :] = ref[d, :tokens, :HEAD]
                values_ref[at : at + tokens, :] = ref[d, :tokens, HEAD:]

    scale = 1.0 / jnp.sqrt(jnp.float32(HEAD))
    for h in range(HEADS_STEP):
        head = slice(h * HEAD, (h + 1) * HEAD)
        scores = lax.dot_general(
            q_ref[:, head], keys_ref[...], (((1,), (1,)), ((), ())), preferred_element_type=jnp.float32
        )
        scores = scores * scale + bias_ref[...]
        top = jnp.max(scores, axis=1, keepdims=True)
        weights = jnp.exp(scores - top)
        total = jnp.sum(weights, axis=1, keepdims=True)
        mixed = jnp.dot(
            weights.astype(jnp.bfloat16), values_ref[...], preferred_element_type=jnp.float32
        )
        out_ref[:, head] = (mixed / total).astype(out_ref.dtype)


def attention(place, queries, mine, other, my_docs):
    tokens = queries.shape[0]
    span = 2 * mine.shape[0] * tokens
    return pl.pallas_call(
        attend,
        grid_spec=pltpu.PrefetchScalarGridSpec(
            num_scalar_prefetch=1,
            grid=(QPK // HEADS_STEP,),
            in_specs=[
                pl.BlockSpec((tokens, HEADS_STEP * HEAD), lambda h, *_: (0, h)),
                IN_VMEM,
                IN_VMEM,
                IN_VMEM,
            ],
            out_specs=pl.BlockSpec((tokens, HEADS_STEP * HEAD), lambda h, *_: (0, h)),
            scratch_shapes=[
                pltpu.VMEM((tokens, span), jnp.float32),
                pltpu.VMEM((span, HEAD), jnp.bfloat16),
                pltpu.VMEM((span, HEAD), jnp.bfloat16),
            ],
        ),
        out_shape=jax.ShapeDtypeStruct(queries.shape, jnp.bfloat16),
        compiler_params=pltpu.CompilerParams(vmem_limit_bytes=16 * MIB),
        name="attend",
    )(place, in_hbm(queries), in_vmem(mine), in_vmem(other), my_docs)


def exchange_x(array):
    return lax.all_to_all(array, "grp", 0, 0, axis_index_groups=OVER_X, tiled=True)


def program(hidden, queries, vis_rows, vis_slot, doc_ids, w_key, w_value):
    tokens = hidden.shape[0]
    cols = 2 * w_key.shape[1]
    where = jnp.stack([lax.axis_index("seq"), lax.axis_index("grp") // NZ])
    rows, piece = packed(where, hidden, vis_rows, w_key, w_value)

    got = lax.all_gather(piece, "grp", axis=0, axis_index_groups=OVER_Z)

    rows = exchange_x(rows)

    mine = lax.all_gather(got, "seq", axis=0, axis_index_groups=OVER_NEAR)
    other = seq_permute(mine, sibling)

    vis = projected_extra(where, rows, mine, other)
    vis = exchange_x(vis)
    text = list(projected_text(where, rows, mine, other))
    for d in (2, 1, 3):
        text[d] = x_permute(text[d], d)
    marks = jnp.broadcast_to(vis_slot.reshape(NS * CAP, 1), (NS * CAP, tokens)).astype(jnp.float32)
    vis = settled(vis, marks)
    vis = lax.all_to_all(vis, "seq", 0, 0, tiled=True)
    docs = jnp.broadcast_to(jnp.tile(doc_ids, (1, cols // tokens)), (8, cols)).astype(jnp.bfloat16)
    block = merged_block(vis, docs, text)

    back = [None] * REACH
    for d in range(REACH, 0, -1):
        back[d - 1] = seq_permute(block, later(d))
    mine = jnp.stack([block, *back])
    other = seq_permute(mine, sibling)
    my_docs = doc_ids.reshape(tokens, 1).astype(jnp.float32)
    return attention(where, queries, mine, other, my_docs)


def solution(mesh):
    return jax.shard_map(
        program,
        mesh=mesh,
        in_specs=(
            P(("grp", "seq"), None),
            P(("grp", "seq"), "tp"),
            P(("grp", "seq"), None, None, None),
            P(("grp", "seq"), None, None),
            P("grp", "seq"),
            P("grp", "tp"),
            P("grp", "tp"),
        ),
        out_specs=P(("grp", "seq"), "tp"),
        check_vma=False,
    )
```

```python
import jax
import jax.numpy as jnp
from jax import lax
from jax.experimental import pallas as pl
from jax.experimental.pallas import tpu as pltpu
from jax.sharding import PartitionSpec as P


HEAD = 128
QPK = 8
CAP = 4
HEADS_STEP = 4
NX = 4
NZ = 4
NLO = 8
NS = 16
NT = 4
REACH = 4
AXES = ("grp", "seq", "tp")
OVER_X = [[x * NZ + z for x in range(NX)] for z in range(NZ)]
OVER_Z = [[x * NZ + z for z in range(NZ)] for x in range(NX)]
NEAR = 2
OVER_NEAR = [
    [(first + i) * 2 + core for i in range(NEAR)] for first in range(0, NLO, NEAR) for core in range(2)
]


def seq_permute(array, move):
    pairs = []
    for g in range(NX * NZ):
        for s in range(NS):
            to = move(s // 2, s % 2)
            if to is None:
                continue
            for t in range(NT):
                pairs.append(((g * NS + s) * NT + t, (g * NS + to[0] * 2 + to[1]) * NT + t))
    return lax.ppermute(array, AXES, pairs)


def x_permute(array, d):
    step, size = NZ * NS * NT, NX * NZ * NS * NT
    return lax.ppermute(array, AXES, [(i, (i + d * step) % size) for i in range(size)])


def sibling(z, c):
    return z, 1 - c


def later(d):
    return lambda z, c: (z + d, c) if z + d < NLO else None


MIB = 1 << 20
IN_VMEM = pl.BlockSpec(memory_space=pltpu.VMEM)


def whole(shape):
    return pl.BlockSpec(shape, lambda *_: (0,) * len(shape))


def in_vmem(array):
    return pltpu.with_memory_space_constraint(array, pltpu.VMEM)


def in_hbm(array):
    return pltpu.with_memory_space_constraint(array, pltpu.HBM)


def pack(place_ref, text_ref, extra_ref, key_ref, value_ref, out_ref, piece_ref, *scratch):
    extra_in, parts, key_part, value_part, text_sem, in_sem, out_sem, piece_sem = scratch
    tokens = text_ref.shape[0]
    width = out_ref.shape[2]
    part = piece_ref.shape[0]
    s = place_ref[0]
    rows = pl.ds(pl.multiple_of(lax.rem(s // 2, NEAR) * part, part), part)
    pieces = [
        pltpu.make_async_copy(key_ref.at[rows], key_part, piece_sem.at[0]),
        pltpu.make_async_copy(value_ref.at[rows], value_part, piece_sem.at[1]),
    ]
    texts, ins, outs = [], [], []
    for q in range(NX):
        cols = pl.ds(q * width, width)
        ins.append(pltpu.make_async_copy(extra_ref.at[0, :, :, cols], extra_in.at[q], in_sem.at[q]))
        texts.append(
            pltpu.make_async_copy(text_ref.at[:, cols], parts.at[q, pl.ds(0, tokens)], text_sem.at[q])
        )
        outs.append(pltpu.make_async_copy(parts.at[q], out_ref.at[q], out_sem.at[q]))
    for q in range(NX):
        ins[q].start()
        texts[q].start()
    for copy in pieces:
        copy.start()
    for q in range(NX):
        ins[q].wait()
        parts[q, tokens:] = extra_in[q].reshape(NS * CAP, width)
        texts[q].wait()
        outs[q].start()
    for copy in pieces:
        copy.wait()
    piece_ref[...] = jnp.where(lax.rem(s, 2) == 0, key_part[...], value_part[...])
    for copy in outs:
        copy.wait()


def packed(place, hidden, vis_rows, w_key, w_value):
    tokens, width = hidden.shape
    count = tokens + NS * CAP
    part = width // NX
    piece = (w_key.shape[0] // NEAR, w_key.shape[1])
    kind = hidden.dtype
    anywhere = pl.BlockSpec(memory_space=pl.ANY)
    return pl.pallas_call(
        pack,
        grid_spec=pltpu.PrefetchScalarGridSpec(
            num_scalar_prefetch=1,
            grid=(1,),
            in_specs=[anywhere] * 4,
            out_specs=[anywhere, IN_VMEM],
            scratch_shapes=[
                pltpu.VMEM((NX, NS, CAP, part), kind),
                pltpu.VMEM((NX, count, part), kind),
                pltpu.VMEM(piece, kind),
                pltpu.VMEM(piece, kind),
                pltpu.SemaphoreType.DMA((NX,)),
                pltpu.SemaphoreType.DMA((NX,)),
                pltpu.SemaphoreType.DMA((NX,)),
                pltpu.SemaphoreType.DMA((2,)),
            ],
        ),
        out_shape=[pltpu.HBM((NX, count, part), kind), pltpu.VMEM(piece, kind)],
        compiler_params=pltpu.CompilerParams(vmem_limit_bytes=16 * MIB),
        name="pack",
    )(place, *map(in_hbm, (hidden, vis_rows, w_key, w_value)))


def order(place_ref, mine_ref, other_ref, weights_ref):
    steps, sources, part, cols = mine_ref.shape
    core = lax.rem(place_ref[0], 2)
    for side, ref in enumerate((mine_ref, other_ref)):
        at = pl.ds(pl.multiple_of(jnp.where(core == side, 0, cols), cols), cols)
        for k in range(steps):
            for z in range(sources):
                row = (z * steps + k) * part
                weights_ref[row : row + part, at] = ref[k, z]


def project_extra(place_ref, rows_ref, mine_ref, other_ref, vis_ref, weights_ref):
    tokens = rows_ref.shape[1] - NS * CAP
    order(place_ref, mine_ref, other_ref, weights_ref)
    weights = weights_ref[...]
    for block in range(NX):
        vis_ref[block] = jnp.dot(
            rows_ref[block, tokens:, :], weights, preferred_element_type=jnp.float32
        )


def projected_extra(place, rows, mine, other):
    blocks, _, part = rows.shape
    cols = 2 * mine.shape[-1]
    vis = pltpu.HBM((blocks, NS * CAP, cols), jnp.float32)
    return pl.pallas_call(
        project_extra,
        grid_spec=pltpu.PrefetchScalarGridSpec(
            num_scalar_prefetch=1,
            grid=(1,),
            in_specs=[IN_VMEM, whole(mine.shape), whole(other.shape)],
            out_specs=pl.BlockSpec(vis.shape, lambda i, _: (0, 0, 0)),
            scratch_shapes=[pltpu.VMEM((part, cols), jnp.bfloat16)],
        ),
        out_shape=vis,
        compiler_params=pltpu.CompilerParams(vmem_limit_bytes=16 * MIB),
        name="project_extra",
    )(place, in_vmem(rows), in_hbm(mine), in_hbm(other))


def project_text(place_ref, rows_ref, mine_ref, other_ref, own_ref, *refs):
    *text_refs, weights_ref = refs
    tokens = own_ref.shape[0]
    x = place_ref[1]
    order(place_ref, mine_ref, other_ref, weights_ref)
    weights = weights_ref[...]
    for d, ref in enumerate((own_ref, *text_refs)):
        ref[...] = jnp.dot(
            rows_ref[lax.rem(x + d, NX), :tokens, :], weights, preferred_element_type=jnp.float32
        )


def projected_text(place, rows, mine, other):
    blocks, count, part = rows.shape
    shape = (count - NS * CAP, 2 * mine.shape[-1])
    return pl.pallas_call(
        project_text,
        grid_spec=pltpu.PrefetchScalarGridSpec(
            num_scalar_prefetch=1,
            grid=(1,),
            in_specs=[IN_VMEM, whole(mine.shape), whole(other.shape)],
            out_specs=[IN_VMEM] + [pl.BlockSpec(shape, lambda i, _: (0, 0))] * (blocks - 1),
            scratch_shapes=[pltpu.VMEM((part, shape[1]), jnp.bfloat16)],
        ),
        out_shape=[pltpu.VMEM(shape, jnp.float32)]
        + [pltpu.HBM(shape, jnp.float32)] * (blocks - 1),
        compiler_params=pltpu.CompilerParams(vmem_limit_bytes=16 * MIB),
        name="project_text",
    )(place, in_vmem(rows), in_hbm(mine), in_hbm(other))


def settle(sums_ref, marks_ref, out_ref):
    cols = sums_ref.shape[-1]
    rows = (sums_ref[0] + sums_ref[1]) + (sums_ref[2] + sums_ref[3])
    for i in range(NS):
        at = slice(i * CAP, (i + 1) * CAP)
        out_ref[i, :, :cols] = rows[at].astype(jnp.bfloat16)
        out_ref[i, :, cols:] = marks_ref[at, :].astype(jnp.bfloat16)


def settled(sums, marks):
    shape = (NS, CAP, sums.shape[-1] + marks.shape[-1])
    return pl.pallas_call(
        settle,
        grid=(1,),
        in_specs=[IN_VMEM] * 2,
        out_specs=pl.BlockSpec(shape, lambda i: (0, 0, 0)),
        out_shape=pltpu.HBM(shape, jnp.bfloat16),
        compiler_params=pltpu.CompilerParams(vmem_limit_bytes=8 * MIB),
        name="settle",
    )(in_vmem(sums), marks)


def merge(vis_ref, docs_ref, *refs):
    *text_refs, out_ref = refs
    tokens, cols = text_refs[0].shape
    text = (text_refs[0][...] + text_refs[1][...]) + (text_refs[2][...] + text_refs[3][...])
    vis = vis_ref[...].reshape(NS * CAP, vis_ref.shape[-1])
    slots = vis[:, cols:].astype(jnp.float32)
    matches = slots == lax.broadcasted_iota(jnp.int32, slots.shape, 1).astype(jnp.float32)
    chooser = matches.astype(jnp.float32).astype(jnp.bfloat16)
    dims = (((0,), (0,)), ((), ()))
    moved = lax.dot_general(chooser, vis[:, :cols], dims, preferred_element_type=jnp.float32)
    ones = jnp.ones((slots.shape[0], cols), jnp.bfloat16)
    used = lax.dot_general(chooser, ones, dims, preferred_element_type=jnp.float32)
    out_ref[:tokens, :] = jnp.where(used > 0.5, moved, text).astype(jnp.bfloat16)
    out_ref[tokens:, :] = docs_ref[...]


def merged_block(vis, docs, text):
    tokens, cols = text[0].shape
    return pl.pallas_call(
        merge,
        in_specs=[IN_VMEM] * (2 + len(text)),
        out_specs=IN_VMEM,
        out_shape=pltpu.VMEM((tokens + docs.shape[0], cols), jnp.bfloat16),
        compiler_params=pltpu.CompilerParams(vmem_limit_bytes=8 * MIB),
        name="merge",
    )(in_vmem(vis), docs, *map(in_vmem, text))


def attend(place_ref, q_ref, mine_ref, other_ref, my_docs_ref, out_ref, bias_ref, keys_ref, values_ref):
    tokens = q_ref.shape[0]
    blocks = mine_ref.shape[0]

    @pl.when(pl.program_id(0) == 0)
    def _():
        s = place_ref[0]
        core, chip = lax.rem(s, 2), s // 2
        my_docs = jnp.broadcast_to(my_docs_ref[...], (tokens, tokens))
        row = lax.broadcasted_iota(jnp.int32, (tokens, tokens), 0) + s * tokens
        col = lax.broadcasted_iota(jnp.int32, (tokens, tokens), 1)
        for side, ref in enumerate((mine_ref, other_ref)):
            for d in range(blocks):
                block = 2 * (chip - d) + (core if side == 0 else 1 - core)
                docs = ref[d, tokens : tokens + 8, :tokens].astype(jnp.float32)[:1]
                spot = col + block * tokens
                allowed = (docs == my_docs) & (spot <= row) & (spot >= 0)
                at = (side * blocks + d) * tokens
                bias_ref[:, at : at + tokens] = jnp.where(allowed, 0.0, -1e30)
                keys_ref[at : at + tokens, :] = ref[d, :tokens, :HEAD]
                values_ref[at : at + tokens, :] = ref[d, :tokens, HEAD:]

    scale = 1.0 / jnp.sqrt(jnp.float32(HEAD))
    for h in range(HEADS_STEP):
        head = slice(h * HEAD, (h + 1) * HEAD)
        scores = lax.dot_general(
            q_ref[:, head], keys_ref[...], (((1,), (1,)), ((), ())), preferred_element_type=jnp.float32
        )
        scores = scores * scale + bias_ref[...]
        top = jnp.max(scores, axis=1, keepdims=True)
        weights = jnp.exp(scores - top)
        total = jnp.sum(weights, axis=1, keepdims=True)
        mixed = jnp.dot(
            weights.astype(jnp.bfloat16), values_ref[...], preferred_element_type=jnp.float32
        )
        out_ref[:, head] = (mixed / total).astype(out_ref.dtype)


def attention(place, queries, mine, other, my_docs):
    tokens = queries.shape[0]
    span = 2 * mine.shape[0] * tokens
    return pl.pallas_call(
        attend,
        grid_spec=pltpu.PrefetchScalarGridSpec(
            num_scalar_prefetch=1,
            grid=(QPK // HEADS_STEP,),
            in_specs=[
                pl.BlockSpec((tokens, HEADS_STEP * HEAD), lambda h, *_: (0, h)),
                IN_VMEM,
                IN_VMEM,
                IN_VMEM,
            ],
            out_specs=pl.BlockSpec((tokens, HEADS_STEP * HEAD), lambda h, *_: (0, h)),
            scratch_shapes=[
                pltpu.VMEM((tokens, span), jnp.float32),
                pltpu.VMEM((span, HEAD), jnp.bfloat16),
                pltpu.VMEM((span, HEAD), jnp.bfloat16),
            ],
        ),
        out_shape=jax.ShapeDtypeStruct(queries.shape, jnp.bfloat16),
        compiler_params=pltpu.CompilerParams(vmem_limit_bytes=16 * MIB),
        name="attend",
    )(place, in_hbm(queries), in_vmem(mine), in_vmem(other), my_docs)


def exchange_x(array):
    return lax.all_to_all(array, "grp", 0, 0, axis_index_groups=OVER_X, tiled=True)


def program(hidden, queries, vis_rows, vis_slot, doc_ids, w_key, w_value):
    tokens = hidden.shape[0]
    cols = 2 * w_key.shape[1]
    where = jnp.stack([lax.axis_index("seq"), lax.axis_index("grp") // NZ])
    rows, piece = packed(where, hidden, vis_rows, w_key, w_value)

    got = lax.all_gather(piece, "grp", axis=0, axis_index_groups=OVER_Z)

    rows = exchange_x(rows)

    mine = lax.all_gather(got, "seq", axis=0, axis_index_groups=OVER_NEAR)
    other = seq_permute(mine, sibling)

    vis = projected_extra(where, rows, mine, other)
    vis = exchange_x(vis)
    text = list(projected_text(where, rows, mine, other))
    for d in (2, 1, 3):
        text[d] = x_permute(text[d], d)
    marks = jnp.broadcast_to(vis_slot.reshape(NS * CAP, 1), (NS * CAP, tokens)).astype(jnp.float32)
    vis = settled(vis, marks)
    vis = lax.all_to_all(vis, "seq", 0, 0, tiled=True)
    docs = jnp.broadcast_to(jnp.tile(doc_ids, (1, cols // tokens)), (8, cols)).astype(jnp.bfloat16)
    block = merged_block(vis, docs, text)

    back = [None] * REACH
    for d in range(REACH, 0, -1):
        back[d - 1] = seq_permute(block, later(d))
    mine = jnp.stack([block, *back])
    other = seq_permute(mine, sibling)
    my_docs = doc_ids.reshape(tokens, 1).astype(jnp.float32)
    return attention(where, queries, mine, other, my_docs)


def solution(mesh):
    return jax.shard_map(
        program,
        mesh=mesh,
        in_specs=(
            P(("grp", "seq"), None),
            P(("grp", "seq"), "tp"),
            P(("grp", "seq"), None, None, None),
            P(("grp", "seq"), None, None),
            P("grp", "seq"),
            P("grp", "tp"),
            P("grp", "tp"),
        ),
        out_specs=P(("grp", "seq"), "tp"),
        check_vma=False,
    )
```

```python
import jax
import jax.numpy as jnp
from jax import lax
from jax.experimental import pallas as pl
from jax.experimental.pallas import tpu as pltpu
from jax.sharding import PartitionSpec as P


HEAD = 128
QPK = 8
CAP = 4
HEADS_STEP = 4
NX = 4
NZ = 4
NLO = 8
NS = 16
NT = 4
REACH = 4
AXES = ("grp", "seq", "tp")
OVER_X = [[x * NZ + z for x in range(NX)] for z in range(NZ)]
OVER_Z = [[x * NZ + z for z in range(NZ)] for x in range(NX)]
NEAR = 2
OVER_NEAR = [[first + i for i in range(2 * NEAR)] for first in range(0, NS, 2 * NEAR)]


def seq_permute(array, move):
    pairs = []
    for g in range(NX * NZ):
        for s in range(NS):
            to = move(s // 2, s % 2)
            if to is None:
                continue
            for t in range(NT):
                pairs.append(((g * NS + s) * NT + t, (g * NS + to[0] * 2 + to[1]) * NT + t))
    return lax.ppermute(array, AXES, pairs)


def x_permute(array, d):
    step, size = NZ * NS * NT, NX * NZ * NS * NT
    return lax.ppermute(array, AXES, [(i, (i + d * step) % size) for i in range(size)])


def sibling(z, c):
    return z, 1 - c


def later(d):
    return lambda z, c: (z + d, c) if z + d < NLO else None


MIB = 1 << 20
IN_VMEM = pl.BlockSpec(memory_space=pltpu.VMEM)


def whole(shape):
    return pl.BlockSpec(shape, lambda *_: (0,) * len(shape))


def in_vmem(array):
    return pltpu.with_memory_space_constraint(array, pltpu.VMEM)


def in_hbm(array):
    return pltpu.with_memory_space_constraint(array, pltpu.HBM)


def pack(place_ref, text_ref, extra_ref, key_ref, value_ref, out_ref, piece_ref, *scratch):
    extra_in, parts, key_part, value_part, text_sem, in_sem, out_sem, piece_sem = scratch
    tokens = text_ref.shape[0]
    width = out_ref.shape[2]
    part = piece_ref.shape[0]
    s = place_ref[0]
    rows = pl.ds(pl.multiple_of(lax.rem(s // 2, NEAR) * part, part), part)
    pieces = [
        pltpu.make_async_copy(key_ref.at[rows], key_part, piece_sem.at[0]),
        pltpu.make_async_copy(value_ref.at[rows], value_part, piece_sem.at[1]),
    ]
    texts, ins, outs = [], [], []
    for q in range(NX):
        cols = pl.ds(q * width, width)
        ins.append(pltpu.make_async_copy(extra_ref.at[0, :, :, cols], extra_in.at[q], in_sem.at[q]))
        texts.append(
            pltpu.make_async_copy(text_ref.at[:, cols], parts.at[q, pl.ds(0, tokens)], text_sem.at[q])
        )
        outs.append(pltpu.make_async_copy(parts.at[q], out_ref.at[q], out_sem.at[q]))
    for q in range(NX):
        ins[q].start()
        texts[q].start()
    for copy in pieces:
        copy.start()
    for q in range(NX):
        ins[q].wait()
        parts[q, tokens:] = extra_in[q].reshape(NS * CAP, width)
        texts[q].wait()
        outs[q].start()
    for copy in pieces:
        copy.wait()
    piece_ref[...] = jnp.where(lax.rem(s, 2) == 0, key_part[...], value_part[...])
    for copy in outs:
        copy.wait()


def packed(place, hidden, vis_rows, w_key, w_value):
    tokens, width = hidden.shape
    count = tokens + NS * CAP
    part = width // NX
    piece = (w_key.shape[0] // NEAR, w_key.shape[1])
    kind = hidden.dtype
    anywhere = pl.BlockSpec(memory_space=pl.ANY)
    return pl.pallas_call(
        pack,
        grid_spec=pltpu.PrefetchScalarGridSpec(
            num_scalar_prefetch=1,
            grid=(1,),
            in_specs=[anywhere] * 4,
            out_specs=[anywhere, IN_VMEM],
            scratch_shapes=[
                pltpu.VMEM((NX, NS, CAP, part), kind),
                pltpu.VMEM((NX, count, part), kind),
                pltpu.VMEM(piece, kind),
                pltpu.VMEM(piece, kind),
                pltpu.SemaphoreType.DMA((NX,)),
                pltpu.SemaphoreType.DMA((NX,)),
                pltpu.SemaphoreType.DMA((NX,)),
                pltpu.SemaphoreType.DMA((2,)),
            ],
        ),
        out_shape=[pltpu.HBM((NX, count, part), kind), pltpu.VMEM(piece, kind)],
        compiler_params=pltpu.CompilerParams(vmem_limit_bytes=16 * MIB),
        name="pack",
    )(place, *map(in_hbm, (hidden, vis_rows, w_key, w_value)))


def project_extra(
    place_ref, rows_ref, key_ref, value_ref, far_ref, vis_ref, out_ref, weights_ref, out_sem
):
    members, sources, part, cols = far_ref.shape
    tokens = rows_ref.shape[1] - NS * CAP
    z = place_ref[2]
    shard = NEAR * part
    own = pl.ds(pl.multiple_of(z * shard, shard), shard)
    weights_ref[own, :cols] = key_ref[...]
    weights_ref[own, cols:] = value_ref[...]
    for i in range(sources):
        first = lax.rem(z + 1 + i, NZ) * shard
        for m in range(members):
            chip, core = divmod(m, 2)
            at = pl.ds(pl.multiple_of(first + chip * part, part), part)
            weights_ref[at, core * cols : (core + 1) * cols] = far_ref[m, i]
    copy = pltpu.make_async_copy(weights_ref, out_ref, out_sem)
    copy.start()
    weights = weights_ref[...]
    for block in range(NX):
        vis_ref[block] = jnp.dot(
            rows_ref[block, tokens:, :], weights, preferred_element_type=jnp.float32
        )
    copy.wait()


def projected_extra(place, rows, w_key, w_value, far):
    blocks, _, part = rows.shape
    cols = 2 * far.shape[-1]
    vis = pltpu.HBM((blocks, NS * CAP, cols), jnp.float32)
    return pl.pallas_call(
        project_extra,
        grid_spec=pltpu.PrefetchScalarGridSpec(
            num_scalar_prefetch=1,
            grid=(1,),
            in_specs=[IN_VMEM, whole(w_key.shape), whole(w_value.shape), IN_VMEM],
            out_specs=[
                pl.BlockSpec(vis.shape, lambda i, _: (0, 0, 0)),
                pl.BlockSpec(memory_space=pl.ANY),
            ],
            scratch_shapes=[pltpu.VMEM((part, cols), jnp.bfloat16), pltpu.SemaphoreType.DMA],
        ),
        out_shape=[vis, pltpu.HBM((part, cols), jnp.bfloat16)],
        compiler_params=pltpu.CompilerParams(vmem_limit_bytes=16 * MIB),
        name="project_extra",
    )(place, in_vmem(rows), in_hbm(w_key), in_hbm(w_value), far)


def project_text(place_ref, rows_ref, weights_ref, own_ref, *text_refs):
    tokens = own_ref.shape[0]
    x = place_ref[1]
    weights = weights_ref[...]
    for d, ref in enumerate((own_ref, *text_refs)):
        ref[...] = jnp.dot(
            rows_ref[lax.rem(x + d, NX), :tokens, :], weights, preferred_element_type=jnp.float32
        )


def projected_text(place, rows, weights):
    blocks, count, _ = rows.shape
    shape = (count - NS * CAP, weights.shape[1])
    return pl.pallas_call(
        project_text,
        grid_spec=pltpu.PrefetchScalarGridSpec(
            num_scalar_prefetch=1,
            grid=(1,),
            in_specs=[IN_VMEM, whole(weights.shape)],
            out_specs=[IN_VMEM] + [pl.BlockSpec(shape, lambda i, _: (0, 0))] * (blocks - 1),
        ),
        out_shape=[pltpu.VMEM(shape, jnp.float32)]
        + [pltpu.HBM(shape, jnp.float32)] * (blocks - 1),
        compiler_params=pltpu.CompilerParams(vmem_limit_bytes=16 * MIB),
        name="project_text",
    )(place, in_vmem(rows), in_hbm(weights))


def settle(sums_ref, marks_ref, out_ref):
    cols = sums_ref.shape[-1]
    rows = (sums_ref[0] + sums_ref[1]) + (sums_ref[2] + sums_ref[3])
    for i in range(NS):
        at = slice(i * CAP, (i + 1) * CAP)
        out_ref[i, :, :cols] = rows[at].astype(jnp.bfloat16)
        out_ref[i, :, cols:] = marks_ref[at, :].astype(jnp.bfloat16)


def settled(sums, marks):
    shape = (NS, CAP, sums.shape[-1] + marks.shape[-1])
    return pl.pallas_call(
        settle,
        grid=(1,),
        in_specs=[IN_VMEM] * 2,
        out_specs=pl.BlockSpec(shape, lambda i: (0, 0, 0)),
        out_shape=pltpu.HBM(shape, jnp.bfloat16),
        compiler_params=pltpu.CompilerParams(vmem_limit_bytes=8 * MIB),
        name="settle",
    )(in_vmem(sums), marks)


def merge(vis_ref, docs_ref, *refs):
    *text_refs, out_ref = refs
    tokens, cols = text_refs[0].shape
    text = (text_refs[0][...] + text_refs[1][...]) + (text_refs[2][...] + text_refs[3][...])
    vis = vis_ref[...].reshape(NS * CAP, vis_ref.shape[-1])
    slots = vis[:, cols:].astype(jnp.float32)
    matches = slots == lax.broadcasted_iota(jnp.int32, slots.shape, 1).astype(jnp.float32)
    chooser = matches.astype(jnp.float32).astype(jnp.bfloat16)
    dims = (((0,), (0,)), ((), ()))
    moved = lax.dot_general(chooser, vis[:, :cols], dims, preferred_element_type=jnp.float32)
    ones = jnp.ones((slots.shape[0], cols), jnp.bfloat16)
    used = lax.dot_general(chooser, ones, dims, preferred_element_type=jnp.float32)
    out_ref[:tokens, :] = jnp.where(used > 0.5, moved, text).astype(jnp.bfloat16)
    out_ref[tokens:, :] = docs_ref[...]


def merged_block(vis, docs, text):
    tokens, cols = text[0].shape
    return pl.pallas_call(
        merge,
        in_specs=[IN_VMEM] * (2 + len(text)),
        out_specs=IN_VMEM,
        out_shape=pltpu.VMEM((tokens + docs.shape[0], cols), jnp.bfloat16),
        compiler_params=pltpu.CompilerParams(vmem_limit_bytes=8 * MIB),
        name="merge",
    )(in_vmem(vis), docs, *map(in_vmem, text))


def attend(place_ref, q_hbm, mine_ref, other_ref, my_docs_ref, out_ref, *scratch):
    bias_ref, keys_ref, values_ref, q_ref, q_sem = scratch
    tokens = q_hbm.shape[0]
    blocks = mine_ref.shape[0]

    @pl.when(pl.program_id(0) == 0)
    def _():
        copy = pltpu.make_async_copy(q_hbm, q_ref, q_sem)
        copy.start()
        s = place_ref[0]
        core, chip = lax.rem(s, 2), s // 2
        my_docs = jnp.broadcast_to(my_docs_ref[...], (tokens, tokens))
        row = lax.broadcasted_iota(jnp.int32, (tokens, tokens), 0) + s * tokens
        col = lax.broadcasted_iota(jnp.int32, (tokens, tokens), 1)
        for side, ref in enumerate((mine_ref, other_ref)):
            for d in range(blocks):
                block = 2 * (chip - d) + (core if side == 0 else 1 - core)
                docs = ref[d, tokens : tokens + 8, :tokens].astype(jnp.float32)[:1]
                spot = col + block * tokens
                allowed = (docs == my_docs) & (spot <= row) & (spot >= 0)
                at = (side * blocks + d) * tokens
                bias_ref[:, at : at + tokens] = jnp.where(allowed, 0.0, -1e30)
                keys_ref[at : at + tokens, :] = ref[d, :tokens, :HEAD]
                values_ref[at : at + tokens, :] = ref[d, :tokens, HEAD:]
        copy.wait()

    scale = 1.0 / jnp.sqrt(jnp.float32(HEAD))
    first = pl.multiple_of(pl.program_id(0) * HEADS_STEP * HEAD, HEAD)
    for h in range(HEADS_STEP):
        head = slice(h * HEAD, (h + 1) * HEAD)
        scores = lax.dot_general(
            q_ref[:, pl.ds(first + h * HEAD, HEAD)], keys_ref[...], (((1,), (1,)), ((), ())), preferred_element_type=jnp.float32
        )
        scores = scores * scale + bias_ref[...]
        top = jnp.max(scores, axis=1, keepdims=True)
        weights = jnp.exp(scores - top)
        total = jnp.sum(weights, axis=1, keepdims=True)
        mixed = jnp.dot(
            weights.astype(jnp.bfloat16), values_ref[...], preferred_element_type=jnp.float32
        )
        out_ref[:, head] = (mixed / total).astype(out_ref.dtype)


def attention(place, queries, mine, other, my_docs):
    tokens = queries.shape[0]
    span = 2 * mine.shape[0] * tokens
    return pl.pallas_call(
        attend,
        grid_spec=pltpu.PrefetchScalarGridSpec(
            num_scalar_prefetch=1,
            grid=(QPK // HEADS_STEP,),
            in_specs=[
                pl.BlockSpec(memory_space=pl.ANY),
                IN_VMEM,
                IN_VMEM,
                IN_VMEM,
            ],
            out_specs=pl.BlockSpec((tokens, HEADS_STEP * HEAD), lambda h, *_: (0, h)),
            scratch_shapes=[
                pltpu.VMEM((tokens, span), jnp.float32),
                pltpu.VMEM((span, HEAD), jnp.bfloat16),
                pltpu.VMEM((span, HEAD), jnp.bfloat16),
                pltpu.VMEM(queries.shape, queries.dtype),
                pltpu.SemaphoreType.DMA,
            ],
        ),
        out_shape=jax.ShapeDtypeStruct(queries.shape, jnp.bfloat16),
        compiler_params=pltpu.CompilerParams(vmem_limit_bytes=16 * MIB),
        name="attend",
    )(place, in_hbm(queries), in_vmem(mine), in_vmem(other), my_docs)


def exchange_x(array):
    return lax.all_to_all(array, "grp", 0, 0, axis_index_groups=OVER_X, tiled=True)


def program(hidden, queries, vis_rows, vis_slot, doc_ids, w_key, w_value):
    tokens = hidden.shape[0]
    cols = 2 * w_key.shape[1]
    grp = lax.axis_index("grp")
    where = jnp.stack([lax.axis_index("seq"), grp // NZ, grp % NZ])
    rows, piece = packed(where, hidden, vis_rows, w_key, w_value)

    got = lax.all_gather(piece, "grp", axis=0, axis_index_groups=OVER_Z)

    rows = exchange_x(rows)

    z = lax.axis_index("grp") % NZ
    far = jnp.stack([lax.dynamic_index_in_dim(got, (z + 1 + i) % NZ, 0, False) for i in range(NZ - 1)])
    far = lax.all_gather(far, "seq", axis=0, axis_index_groups=OVER_NEAR)

    vis, weights = projected_extra(where, rows, w_key, w_value, far)
    vis = exchange_x(vis)
    text = list(projected_text(where, rows, weights))
    for d in (2, 1, 3):
        text[d] = x_permute(text[d], d)
    marks = jnp.broadcast_to(vis_slot.reshape(NS * CAP, 1), (NS * CAP, tokens)).astype(jnp.float32)
    vis = settled(vis, marks)
    vis = lax.all_to_all(vis, "seq", 0, 0, tiled=True)
    docs = jnp.broadcast_to(jnp.tile(doc_ids, (1, cols // tokens)), (8, cols)).astype(jnp.bfloat16)
    block = merged_block(vis, docs, text)

    back = [None] * REACH
    for d in range(REACH, 0, -1):
        back[d - 1] = seq_permute(block, later(d))
    mine = jnp.stack([block, *back])
    other = seq_permute(mine, sibling)
    my_docs = doc_ids.reshape(tokens, 1).astype(jnp.float32)
    return attention(where, queries, mine, other, my_docs)


def solution(mesh):
    return jax.shard_map(
        program,
        mesh=mesh,
        in_specs=(
            P(("grp", "seq"), None),
            P(("grp", "seq"), "tp"),
            P(("grp", "seq"), None, None, None),
            P(("grp", "seq"), None, None),
            P("grp", "seq"),
            P("grp", "tp"),
            P("grp", "tp"),
        ),
        out_specs=P(("grp", "seq"), "tp"),
        check_vma=False,
    )
```

```python
import jax
import jax.numpy as jnp
from jax import lax
from jax.experimental import pallas as pl
from jax.experimental.pallas import tpu as pltpu
from jax.sharding import PartitionSpec as P


HEAD = 128
QPK = 8
CAP = 4
LOG2E = 1.4426950408889634
HEADS_STEP = 4
NX = 4
NZ = 4
NLO = 8
NS = 16
NT = 4
REACH = 4
AXES = ("grp", "seq", "tp")
OVER_X = [[x * NZ + z for x in range(NX)] for z in range(NZ)]
OVER_Z = [[x * NZ + z for z in range(NZ)] for x in range(NX)]
NEAR = 2
OVER_NEAR = [[first + i for i in range(2 * NEAR)] for first in range(0, NS, 2 * NEAR)]


def seq_permute(array, move):
    pairs = []
    for g in range(NX * NZ):
        for s in range(NS):
            to = move(s // 2, s % 2)
            if to is None:
                continue
            for t in range(NT):
                pairs.append(((g * NS + s) * NT + t, (g * NS + to[0] * 2 + to[1]) * NT + t))
    return lax.ppermute(array, AXES, pairs)


def x_permute(array, d):
    step, size = NZ * NS * NT, NX * NZ * NS * NT
    return lax.ppermute(array, AXES, [(i, (i + d * step) % size) for i in range(size)])


def sibling(z, c):
    return z, 1 - c


def later(d):
    return lambda z, c: (z + d, c) if z + d < NLO else None


MIB = 1 << 20
IN_VMEM = pl.BlockSpec(memory_space=pltpu.VMEM)


def whole(shape):
    return pl.BlockSpec(shape, lambda *_: (0,) * len(shape))


def in_vmem(array):
    return pltpu.with_memory_space_constraint(array, pltpu.VMEM)


def in_hbm(array):
    return pltpu.with_memory_space_constraint(array, pltpu.HBM)


def pack(place_ref, text_ref, extra_ref, key_ref, value_ref, out_ref, piece_ref, *scratch):
    extra_in, parts, key_part, value_part, text_sem, in_sem, out_sem, piece_sem = scratch
    tokens = text_ref.shape[0]
    width = out_ref.shape[2]
    part = piece_ref.shape[0]
    s = place_ref[0]
    rows = pl.ds(pl.multiple_of(lax.rem(s // 2, NEAR) * part, part), part)
    pieces = [
        pltpu.make_async_copy(key_ref.at[rows], key_part, piece_sem.at[0]),
        pltpu.make_async_copy(value_ref.at[rows], value_part, piece_sem.at[1]),
    ]
    texts, ins, outs = [], [], []
    for q in range(NX):
        cols = pl.ds(q * width, width)
        ins.append(pltpu.make_async_copy(extra_ref.at[0, :, :, cols], extra_in.at[q], in_sem.at[q]))
        texts.append(
            pltpu.make_async_copy(text_ref.at[:, cols], parts.at[q, pl.ds(0, tokens)], text_sem.at[q])
        )
        outs.append(pltpu.make_async_copy(parts.at[q], out_ref.at[q], out_sem.at[q]))
    for q in range(NX):
        ins[q].start()
        texts[q].start()
    for copy in pieces:
        copy.start()
    for q in range(NX):
        ins[q].wait()
        parts[q, tokens:] = extra_in[q].reshape(NS * CAP, width)
        texts[q].wait()
        outs[q].start()
    for copy in pieces:
        copy.wait()
    piece_ref[...] = jnp.where(lax.rem(s, 2) == 0, key_part[...], value_part[...])
    for copy in outs:
        copy.wait()


def packed(place, hidden, vis_rows, w_key, w_value):
    tokens, width = hidden.shape
    count = tokens + NS * CAP
    part = width // NX
    piece = (w_key.shape[0] // NEAR, w_key.shape[1])
    kind = hidden.dtype
    anywhere = pl.BlockSpec(memory_space=pl.ANY)
    return pl.pallas_call(
        pack,
        grid_spec=pltpu.PrefetchScalarGridSpec(
            num_scalar_prefetch=1,
            grid=(1,),
            in_specs=[anywhere] * 4,
            out_specs=[anywhere, IN_VMEM],
            scratch_shapes=[
                pltpu.VMEM((NX, NS, CAP, part), kind),
                pltpu.VMEM((NX, count, part), kind),
                pltpu.VMEM(piece, kind),
                pltpu.VMEM(piece, kind),
                pltpu.SemaphoreType.DMA((NX,)),
                pltpu.SemaphoreType.DMA((NX,)),
                pltpu.SemaphoreType.DMA((NX,)),
                pltpu.SemaphoreType.DMA((2,)),
            ],
        ),
        out_shape=[pltpu.HBM((NX, count, part), kind), pltpu.VMEM(piece, kind)],
        compiler_params=pltpu.CompilerParams(vmem_limit_bytes=16 * MIB),
        name="pack",
    )(place, *map(in_hbm, (hidden, vis_rows, w_key, w_value)))


def project_extra(
    place_ref, rows_ref, key_ref, value_ref, far_ref, vis_ref, out_ref, weights_ref, in_sem, out_sem
):
    members, sources, part, cols = far_ref.shape
    tokens = rows_ref.shape[1] - NS * CAP
    z = place_ref[2]
    shard = NEAR * part
    own = pl.ds(pl.multiple_of(z * shard, shard), shard)
    copies = [(key_ref, own, 0), (value_ref, own, 1)]
    for i in range(sources):
        first = lax.rem(z + 1 + i, NZ) * shard
        for m in range(members):
            chip, core = divmod(m, 2)
            at = pl.ds(pl.multiple_of(first + chip * part, part), part)
            copies.append((far_ref.at[m, i], at, core))
    copies = [
        pltpu.make_async_copy(
            ref, weights_ref.at[at, pl.ds(side * cols, cols)], in_sem.at[k]
        )
        for k, (ref, at, side) in enumerate(copies)
    ]
    for copy in copies:
        copy.start()
    for copy in copies:
        copy.wait()
    copy = pltpu.make_async_copy(weights_ref, out_ref, out_sem)
    copy.start()
    weights = weights_ref[...]
    for block in range(NX):
        vis_ref[block] = jnp.dot(
            rows_ref[block, tokens:, :], weights, preferred_element_type=jnp.float32
        )
    copy.wait()


def projected_extra(place, rows, w_key, w_value, far):
    blocks, _, part = rows.shape
    cols = 2 * far.shape[-1]
    vis = pltpu.HBM((blocks, NS * CAP, cols), jnp.float32)
    return pl.pallas_call(
        project_extra,
        grid_spec=pltpu.PrefetchScalarGridSpec(
            num_scalar_prefetch=1,
            grid=(1,),
            in_specs=[IN_VMEM] + [pl.BlockSpec(memory_space=pl.ANY)] * 3,
            out_specs=[
                pl.BlockSpec(vis.shape, lambda i, _: (0, 0, 0)),
                pl.BlockSpec(memory_space=pl.ANY),
            ],
            scratch_shapes=[
                pltpu.VMEM((part, cols), jnp.bfloat16),
                pltpu.SemaphoreType.DMA((2 + far.shape[0] * far.shape[1],)),
                pltpu.SemaphoreType.DMA,
            ],
        ),
        out_shape=[vis, pltpu.HBM((part, cols), jnp.bfloat16)],
        compiler_params=pltpu.CompilerParams(vmem_limit_bytes=16 * MIB),
        name="project_extra",
    )(place, in_vmem(rows), in_hbm(w_key), in_hbm(w_value), in_hbm(far))


def project_text(place_ref, rows_ref, weights_ref, own_ref, *text_refs):
    tokens = own_ref.shape[0]
    x = place_ref[1]
    weights = weights_ref[...]
    for d, ref in enumerate((own_ref, *text_refs)):
        ref[...] = jnp.dot(
            rows_ref[lax.rem(x + d, NX), :tokens, :], weights, preferred_element_type=jnp.float32
        )


def projected_text(place, rows, weights):
    blocks, count, _ = rows.shape
    shape = (count - NS * CAP, weights.shape[1])
    return pl.pallas_call(
        project_text,
        grid_spec=pltpu.PrefetchScalarGridSpec(
            num_scalar_prefetch=1,
            grid=(1,),
            in_specs=[IN_VMEM, whole(weights.shape)],
            out_specs=[IN_VMEM] + [pl.BlockSpec(shape, lambda i, _: (0, 0))] * (blocks - 1),
        ),
        out_shape=[pltpu.VMEM(shape, jnp.float32)]
        + [pltpu.HBM(shape, jnp.float32)] * (blocks - 1),
        compiler_params=pltpu.CompilerParams(vmem_limit_bytes=16 * MIB),
        name="project_text",
    )(place, in_vmem(rows), in_hbm(weights))


def settle(sums_ref, marks_ref, out_ref):
    cols = sums_ref.shape[-1]
    rows = (sums_ref[0] + sums_ref[1]) + (sums_ref[2] + sums_ref[3])
    for i in range(NS):
        at = slice(i * CAP, (i + 1) * CAP)
        out_ref[i, :, :cols] = rows[at].astype(jnp.bfloat16)
        out_ref[i, :, cols:] = marks_ref[at, :].astype(jnp.bfloat16)


def settled(sums, marks):
    shape = (NS, CAP, sums.shape[-1] + marks.shape[-1])
    return pl.pallas_call(
        settle,
        grid=(1,),
        in_specs=[IN_VMEM] * 2,
        out_specs=pl.BlockSpec(shape, lambda i: (0, 0, 0)),
        out_shape=pltpu.HBM(shape, jnp.bfloat16),
        compiler_params=pltpu.CompilerParams(vmem_limit_bytes=8 * MIB),
        name="settle",
    )(in_vmem(sums), marks)


def merge(vis_ref, docs_ref, *refs):
    *text_refs, out_ref = refs
    tokens, cols = text_refs[0].shape
    text = (text_refs[0][...] + text_refs[1][...]) + (text_refs[2][...] + text_refs[3][...])
    vis = vis_ref[...].reshape(NS * CAP, vis_ref.shape[-1])
    slots = vis[:, cols:].astype(jnp.float32)
    matches = slots == lax.broadcasted_iota(jnp.int32, slots.shape, 1).astype(jnp.float32)
    chooser = matches.astype(jnp.float32).astype(jnp.bfloat16)
    dims = (((0,), (0,)), ((), ()))
    moved = lax.dot_general(chooser, vis[:, :cols], dims, preferred_element_type=jnp.float32)
    ones = jnp.ones((slots.shape[0], cols), jnp.bfloat16)
    used = lax.dot_general(chooser, ones, dims, preferred_element_type=jnp.float32)
    out_ref[:tokens, :] = jnp.where(used > 0.5, moved, text).astype(jnp.bfloat16)
    out_ref[tokens:, :] = docs_ref[...]


def merged_block(vis, docs, text):
    tokens, cols = text[0].shape
    return pl.pallas_call(
        merge,
        in_specs=[IN_VMEM] * (2 + len(text)),
        out_specs=IN_VMEM,
        out_shape=pltpu.VMEM((tokens + docs.shape[0], cols), jnp.bfloat16),
        compiler_params=pltpu.CompilerParams(vmem_limit_bytes=8 * MIB),
        name="merge",
    )(in_vmem(vis), docs, *map(in_vmem, text))


def attend(place_ref, q_hbm, mine_ref, other_ref, my_docs_ref, out_ref, *scratch):
    bias_ref, keys_ref, values_ref, q_ref, q_rows, q_sem = scratch
    tokens = q_hbm.shape[0]
    blocks = mine_ref.shape[0]

    @pl.when(pl.program_id(0) == 0)
    def _():
        copy = pltpu.make_async_copy(q_hbm, q_ref, q_sem)
        copy.start()
        s = place_ref[0]
        core, chip = lax.rem(s, 2), s // 2
        my_docs = jnp.broadcast_to(my_docs_ref[...], (tokens, tokens))
        row = lax.broadcasted_iota(jnp.int32, (tokens, tokens), 0) + s * tokens
        col = lax.broadcasted_iota(jnp.int32, (tokens, tokens), 1)
        for side, ref in enumerate((mine_ref, other_ref)):
            for d in range(blocks):
                block = 2 * (chip - d) + (core if side == 0 else 1 - core)
                docs = ref[d, tokens : tokens + 8, :tokens].astype(jnp.float32)[:1]
                spot = col + block * tokens
                allowed = (docs == my_docs) & (spot <= row) & (spot >= 0)
                at = (side * blocks + d) * tokens
                bias_ref[:, at : at + tokens] = jnp.where(allowed, 0.0, -1e30)
                keys_ref[at : at + tokens, :] = ref[d, :tokens, :HEAD]
                values_ref[at : at + tokens, :] = ref[d, :tokens, HEAD:]
        copy.wait()
        for h in range(QPK):
            q_rows[h * tokens : (h + 1) * tokens, :] = q_ref[:, h * HEAD : (h + 1) * HEAD]

    scale = jnp.float32(LOG2E) / jnp.sqrt(jnp.float32(HEAD))
    rows = HEADS_STEP * tokens
    at = pl.ds(pl.multiple_of(pl.program_id(0) * rows, rows), rows)
    scores = lax.dot_general(
        q_rows[at, :], keys_ref[...], (((1,), (1,)), ((), ())), preferred_element_type=jnp.float32
    )
    scores = scores.reshape(HEADS_STEP, tokens, -1) * scale + bias_ref[...][None]
    top = jnp.max(scores, axis=2, keepdims=True)
    weights = jnp.exp2(scores - top)
    total = jnp.sum(weights, axis=2, keepdims=True)
    mixed = jnp.dot(
        weights.astype(jnp.bfloat16).reshape(rows, -1),
        values_ref[...],
        preferred_element_type=jnp.float32,
    )
    mixed = mixed.reshape(HEADS_STEP, tokens, HEAD) / total
    for h in range(HEADS_STEP):
        out_ref[:, h * HEAD : (h + 1) * HEAD] = mixed[h].astype(out_ref.dtype)


def attention(place, queries, mine, other, my_docs):
    tokens = queries.shape[0]
    span = 2 * mine.shape[0] * tokens
    return pl.pallas_call(
        attend,
        grid_spec=pltpu.PrefetchScalarGridSpec(
            num_scalar_prefetch=1,
            grid=(QPK // HEADS_STEP,),
            in_specs=[
                pl.BlockSpec(memory_space=pl.ANY),
                IN_VMEM,
                IN_VMEM,
                IN_VMEM,
            ],
            out_specs=pl.BlockSpec((tokens, HEADS_STEP * HEAD), lambda h, *_: (0, h)),
            scratch_shapes=[
                pltpu.VMEM((tokens, span), jnp.float32),
                pltpu.VMEM((span, HEAD), jnp.bfloat16),
                pltpu.VMEM((span, HEAD), jnp.bfloat16),
                pltpu.VMEM(queries.shape, queries.dtype),
                pltpu.VMEM((QPK * tokens, HEAD), queries.dtype),
                pltpu.SemaphoreType.DMA,
            ],
        ),
        out_shape=jax.ShapeDtypeStruct(queries.shape, jnp.bfloat16),
        compiler_params=pltpu.CompilerParams(vmem_limit_bytes=16 * MIB),
        name="attend",
    )(place, in_hbm(queries), in_vmem(mine), in_vmem(other), my_docs)


def exchange_x(array):
    return lax.all_to_all(array, "grp", 0, 0, axis_index_groups=OVER_X, tiled=True)


def program(hidden, queries, vis_rows, vis_slot, doc_ids, w_key, w_value):
    tokens = hidden.shape[0]
    cols = 2 * w_key.shape[1]
    grp = lax.axis_index("grp")
    where = jnp.stack([lax.axis_index("seq"), grp // NZ, grp % NZ])
    rows, piece = packed(where, hidden, vis_rows, w_key, w_value)

    got = lax.all_gather(piece, "grp", axis=0, axis_index_groups=OVER_Z)

    rows = exchange_x(rows)

    z = lax.axis_index("grp") % NZ
    far = jnp.stack([lax.dynamic_index_in_dim(got, (z + 1 + i) % NZ, 0, False) for i in range(NZ - 1)])
    far = lax.all_gather(far, "seq", axis=0, axis_index_groups=OVER_NEAR)

    vis, weights = projected_extra(where, rows, w_key, w_value, far)
    vis = exchange_x(vis)
    text = list(projected_text(where, rows, weights))
    for d in (2, 1, 3):
        text[d] = x_permute(text[d], d)
    marks = jnp.broadcast_to(vis_slot.reshape(NS * CAP, 1), (NS * CAP, tokens)).astype(jnp.float32)
    vis = settled(vis, marks)
    vis = lax.all_to_all(vis, "seq", 0, 0, tiled=True)
    docs = jnp.broadcast_to(jnp.tile(doc_ids, (1, cols // tokens)), (8, cols)).astype(jnp.bfloat16)
    block = merged_block(vis, docs, text)

    back = [None] * REACH
    for d in range(REACH, 0, -1):
        back[d - 1] = seq_permute(block, later(d))
    mine = jnp.stack([block, *back])
    other = seq_permute(mine, sibling)
    my_docs = doc_ids.reshape(tokens, 1).astype(jnp.float32)
    return attention(where, queries, mine, other, my_docs)


def solution(mesh):
    return jax.shard_map(
        program,
        mesh=mesh,
        in_specs=(
            P(("grp", "seq"), None),
            P(("grp", "seq"), "tp"),
            P(("grp", "seq"), None, None, None),
            P(("grp", "seq"), None, None),
            P("grp", "seq"),
            P("grp", "tp"),
            P("grp", "tp"),
        ),
        out_specs=P(("grp", "seq"), "tp"),
        check_vma=False,
    )
```

```python
import jax
import jax.numpy as jnp
from jax import lax
from jax.experimental import pallas as pl
from jax.experimental.pallas import tpu as pltpu
from jax.sharding import PartitionSpec as P


HEAD = 128
QPK = 8
CAP = 4
LOG2E = 1.4426950408889634
HEADS_STEP = 4
NX = 4
NZ = 4
NLO = 8
NS = 16
NT = 4
REACH = 4
AXES = ("grp", "seq", "tp")
OVER_X = [[x * NZ + z for x in range(NX)] for z in range(NZ)]
OVER_Z = [[x * NZ + z for z in range(NZ)] for x in range(NX)]
NEAR = 2
OVER_NEAR = [[first + i for i in range(2 * NEAR)] for first in range(0, NS, 2 * NEAR)]


def seq_permute(array, move):
    pairs = []
    for g in range(NX * NZ):
        for s in range(NS):
            to = move(s // 2, s % 2)
            if to is None:
                continue
            for t in range(NT):
                pairs.append(((g * NS + s) * NT + t, (g * NS + to[0] * 2 + to[1]) * NT + t))
    return lax.ppermute(array, AXES, pairs)


def x_permute(array, d):
    step, size = NZ * NS * NT, NX * NZ * NS * NT
    return lax.ppermute(array, AXES, [(i, (i + d * step) % size) for i in range(size)])


def sibling(z, c):
    return z, 1 - c


def later(d):
    return lambda z, c: (z + d, c) if z + d < NLO else None


MIB = 1 << 20
IN_VMEM = pl.BlockSpec(memory_space=pltpu.VMEM)


def whole(shape):
    return pl.BlockSpec(shape, lambda *_: (0,) * len(shape))


def in_vmem(array):
    return pltpu.with_memory_space_constraint(array, pltpu.VMEM)


def in_hbm(array):
    return pltpu.with_memory_space_constraint(array, pltpu.HBM)


def pack(place_ref, text_ref, extra_ref, key_ref, value_ref, out_ref, piece_ref, *scratch):
    extra_in, parts, key_part, value_part, text_sem, in_sem, out_sem, piece_sem = scratch
    tokens = text_ref.shape[0]
    width = out_ref.shape[2]
    part = piece_ref.shape[0]
    s = place_ref[0]
    rows = pl.ds(pl.multiple_of(lax.rem(s // 2, NEAR) * part, part), part)
    pieces = [
        pltpu.make_async_copy(key_ref.at[rows], key_part, piece_sem.at[0]),
        pltpu.make_async_copy(value_ref.at[rows], value_part, piece_sem.at[1]),
    ]
    texts, ins, outs = [], [], []
    for q in range(NX):
        cols = pl.ds(q * width, width)
        ins.append(pltpu.make_async_copy(extra_ref.at[0, :, :, cols], extra_in.at[q], in_sem.at[q]))
        texts.append(
            pltpu.make_async_copy(text_ref.at[:, cols], parts.at[q, pl.ds(0, tokens)], text_sem.at[q])
        )
        outs.append(pltpu.make_async_copy(parts.at[q], out_ref.at[q], out_sem.at[q]))
    for q in range(NX):
        ins[q].start()
        texts[q].start()
    for copy in pieces:
        copy.start()
    for q in range(NX):
        ins[q].wait()
        parts[q, tokens:] = extra_in[q].reshape(NS * CAP, width)
        texts[q].wait()
        outs[q].start()
    for copy in pieces:
        copy.wait()
    piece_ref[...] = jnp.where(lax.rem(s, 2) == 0, key_part[...], value_part[...])
    for copy in outs:
        copy.wait()


def packed(place, hidden, vis_rows, w_key, w_value):
    tokens, width = hidden.shape
    count = tokens + NS * CAP
    part = width // NX
    piece = (w_key.shape[0] // NEAR, w_key.shape[1])
    kind = hidden.dtype
    anywhere = pl.BlockSpec(memory_space=pl.ANY)
    return pl.pallas_call(
        pack,
        grid_spec=pltpu.PrefetchScalarGridSpec(
            num_scalar_prefetch=1,
            grid=(1,),
            in_specs=[anywhere] * 4,
            out_specs=[anywhere, IN_VMEM],
            scratch_shapes=[
                pltpu.VMEM((NX, NS, CAP, part), kind),
                pltpu.VMEM((NX, count, part), kind),
                pltpu.VMEM(piece, kind),
                pltpu.VMEM(piece, kind),
                pltpu.SemaphoreType.DMA((NX,)),
                pltpu.SemaphoreType.DMA((NX,)),
                pltpu.SemaphoreType.DMA((NX,)),
                pltpu.SemaphoreType.DMA((2,)),
            ],
        ),
        out_shape=[pltpu.HBM((NX, count, part), kind), pltpu.VMEM(piece, kind)],
        compiler_params=pltpu.CompilerParams(vmem_limit_bytes=16 * MIB),
        name="pack",
    )(place, *map(in_hbm, (hidden, vis_rows, w_key, w_value)))


def project_extra(
    place_ref, rows_ref, key_ref, value_ref, far_ref, vis_ref, out_ref, weights_ref, in_sem, out_sem
):
    members, sources, part, cols = far_ref.shape
    tokens = rows_ref.shape[1] - NS * CAP
    z = place_ref[2]
    shard = NEAR * part
    own = pl.ds(pl.multiple_of(z * shard, shard), shard)
    copies = [(key_ref, own, 0), (value_ref, own, 1)]
    for i in range(sources):
        first = lax.rem(z + 1 + i, NZ) * shard
        for m in range(members):
            chip, core = divmod(m, 2)
            at = pl.ds(pl.multiple_of(first + chip * part, part), part)
            copies.append((far_ref.at[m, i], at, core))
    copies = [
        pltpu.make_async_copy(
            ref, weights_ref.at[at, pl.ds(side * cols, cols)], in_sem.at[k]
        )
        for k, (ref, at, side) in enumerate(copies)
    ]
    for copy in copies:
        copy.start()
    for copy in copies:
        copy.wait()
    copy = pltpu.make_async_copy(weights_ref, out_ref, out_sem)
    copy.start()
    weights = weights_ref[...]
    for block in range(NX):
        vis_ref[block] = jnp.dot(
            rows_ref[block, tokens:, :], weights, preferred_element_type=jnp.float32
        )
    copy.wait()


def projected_extra(place, rows, w_key, w_value, far):
    blocks, _, part = rows.shape
    cols = 2 * far.shape[-1]
    vis = pltpu.HBM((blocks, NS * CAP, cols), jnp.float32)
    return pl.pallas_call(
        project_extra,
        grid_spec=pltpu.PrefetchScalarGridSpec(
            num_scalar_prefetch=1,
            grid=(1,),
            in_specs=[IN_VMEM] + [pl.BlockSpec(memory_space=pl.ANY)] * 3,
            out_specs=[
                pl.BlockSpec(vis.shape, lambda i, _: (0, 0, 0)),
                pl.BlockSpec(memory_space=pl.ANY),
            ],
            scratch_shapes=[
                pltpu.VMEM((part, cols), jnp.bfloat16),
                pltpu.SemaphoreType.DMA((2 + far.shape[0] * far.shape[1],)),
                pltpu.SemaphoreType.DMA,
            ],
        ),
        out_shape=[vis, pltpu.HBM((part, cols), jnp.bfloat16)],
        compiler_params=pltpu.CompilerParams(vmem_limit_bytes=16 * MIB),
        name="project_extra",
    )(place, in_vmem(rows), in_hbm(w_key), in_hbm(w_value), in_hbm(far))


def project_text(place_ref, rows_ref, weights_ref, own_ref, *text_refs):
    tokens = own_ref.shape[0]
    x = place_ref[1]
    weights = weights_ref[...]
    for d, ref in enumerate((own_ref, *text_refs)):
        ref[...] = jnp.dot(
            rows_ref[lax.rem(x + d, NX), :tokens, :], weights, preferred_element_type=jnp.float32
        )


def projected_text(place, rows, weights):
    blocks, count, _ = rows.shape
    shape = (count - NS * CAP, weights.shape[1])
    return pl.pallas_call(
        project_text,
        grid_spec=pltpu.PrefetchScalarGridSpec(
            num_scalar_prefetch=1,
            grid=(1,),
            in_specs=[IN_VMEM, whole(weights.shape)],
            out_specs=[IN_VMEM] + [pl.BlockSpec(shape, lambda i, _: (0, 0))] * (blocks - 1),
        ),
        out_shape=[pltpu.VMEM(shape, jnp.float32)]
        + [pltpu.HBM(shape, jnp.float32)] * (blocks - 1),
        compiler_params=pltpu.CompilerParams(vmem_limit_bytes=16 * MIB),
        name="project_text",
    )(place, in_vmem(rows), in_hbm(weights))


def settle(sums_ref, marks_ref, out_ref):
    cols = sums_ref.shape[-1]
    rows = (sums_ref[0] + sums_ref[1]) + (sums_ref[2] + sums_ref[3])
    for i in range(NS):
        at = slice(i * CAP, (i + 1) * CAP)
        out_ref[i, :, :cols] = rows[at].astype(jnp.bfloat16)
        out_ref[i, :, cols:] = marks_ref[at, :].astype(jnp.bfloat16)


def settled(sums, marks):
    shape = (NS, CAP, sums.shape[-1] + marks.shape[-1])
    return pl.pallas_call(
        settle,
        grid=(1,),
        in_specs=[IN_VMEM] * 2,
        out_specs=pl.BlockSpec(shape, lambda i: (0, 0, 0)),
        out_shape=pltpu.HBM(shape, jnp.bfloat16),
        compiler_params=pltpu.CompilerParams(vmem_limit_bytes=8 * MIB),
        name="settle",
    )(in_vmem(sums), marks)


def merge(vis_ref, docs_ref, *refs):
    *text_refs, out_ref = refs
    tokens, cols = text_refs[0].shape
    text = (text_refs[0][...] + text_refs[1][...]) + (text_refs[2][...] + text_refs[3][...])
    vis = vis_ref[...].reshape(NS * CAP, vis_ref.shape[-1])
    slots = vis[:, cols:].astype(jnp.float32)
    matches = slots == lax.broadcasted_iota(jnp.int32, slots.shape, 1).astype(jnp.float32)
    chooser = matches.astype(jnp.float32).astype(jnp.bfloat16)
    dims = (((0,), (0,)), ((), ()))
    moved = lax.dot_general(chooser, vis[:, :cols], dims, preferred_element_type=jnp.float32)
    ones = jnp.ones((slots.shape[0], cols), jnp.bfloat16)
    used = lax.dot_general(chooser, ones, dims, preferred_element_type=jnp.float32)
    out_ref[:tokens, :] = jnp.where(used > 0.5, moved, text).astype(jnp.bfloat16)
    out_ref[tokens:, :] = docs_ref[...]


def merged_block(vis, docs, text):
    tokens, cols = text[0].shape
    return pl.pallas_call(
        merge,
        in_specs=[IN_VMEM] * (2 + len(text)),
        out_specs=IN_VMEM,
        out_shape=pltpu.VMEM((tokens + docs.shape[0], cols), jnp.bfloat16),
        compiler_params=pltpu.CompilerParams(vmem_limit_bytes=8 * MIB),
        name="merge",
    )(in_vmem(vis), docs, *map(in_vmem, text))


def attend(place_ref, q_hbm, mine_ref, other_ref, my_docs_ref, out_ref, *scratch):
    bias_ref, keys_ref, values_ref, q_ref, q_sem = scratch
    tokens = q_hbm.shape[0]
    blocks = mine_ref.shape[0]

    @pl.when(pl.program_id(0) == 0)
    def _():
        copy = pltpu.make_async_copy(q_hbm, q_ref, q_sem)
        copy.start()
        s = place_ref[0]
        core, chip = lax.rem(s, 2), s // 2
        my_docs = jnp.broadcast_to(my_docs_ref[...], (tokens, tokens))
        row = lax.broadcasted_iota(jnp.int32, (tokens, tokens), 0) + s * tokens
        col = lax.broadcasted_iota(jnp.int32, (tokens, tokens), 1)
        for side, ref in enumerate((mine_ref, other_ref)):
            for d in range(blocks):
                block = 2 * (chip - d) + (core if side == 0 else 1 - core)
                docs = ref[d, tokens : tokens + 8, :tokens].astype(jnp.float32)[:1]
                spot = col + block * tokens
                allowed = (docs == my_docs) & (spot <= row) & (spot >= 0)
                at = (side * blocks + d) * tokens
                bias_ref[:, at : at + tokens] = jnp.where(allowed, 0.0, -1e30)
                keys_ref[at : at + tokens, :] = ref[d, :tokens, :HEAD]
                values_ref[at : at + tokens, :] = ref[d, :tokens, HEAD:]
        copy.wait()

    scale = jnp.float32(LOG2E) / jnp.sqrt(jnp.float32(HEAD))
    first = pl.multiple_of(pl.program_id(0) * HEADS_STEP * HEAD, HEAD)
    for h in range(HEADS_STEP):
        head = slice(h * HEAD, (h + 1) * HEAD)
        scores = lax.dot_general(
            q_ref[:, pl.ds(first + h * HEAD, HEAD)], keys_ref[...], (((1,), (1,)), ((), ())), preferred_element_type=jnp.float32
        )
        scores = scores * scale + bias_ref[...]
        top = jnp.max(scores, axis=1, keepdims=True)
        weights = jnp.exp2(scores - top)
        total = jnp.sum(weights, axis=1, keepdims=True)
        mixed = jnp.dot(
            weights.astype(jnp.bfloat16), values_ref[...], preferred_element_type=jnp.float32
        )
        out_ref[:, head] = (mixed / total).astype(out_ref.dtype)


def attention(place, queries, mine, other, my_docs):
    tokens = queries.shape[0]
    span = 2 * mine.shape[0] * tokens
    return pl.pallas_call(
        attend,
        grid_spec=pltpu.PrefetchScalarGridSpec(
            num_scalar_prefetch=1,
            grid=(QPK // HEADS_STEP,),
            in_specs=[
                pl.BlockSpec(memory_space=pl.ANY),
                IN_VMEM,
                IN_VMEM,
                IN_VMEM,
            ],
            out_specs=pl.BlockSpec((tokens, HEADS_STEP * HEAD), lambda h, *_: (0, h)),
            scratch_shapes=[
                pltpu.VMEM((tokens, span), jnp.float32),
                pltpu.VMEM((span, HEAD), jnp.bfloat16),
                pltpu.VMEM((span, HEAD), jnp.bfloat16),
                pltpu.VMEM(queries.shape, queries.dtype),
                pltpu.SemaphoreType.DMA,
            ],
        ),
        out_shape=jax.ShapeDtypeStruct(queries.shape, jnp.bfloat16),
        compiler_params=pltpu.CompilerParams(vmem_limit_bytes=16 * MIB),
        name="attend",
    )(place, in_hbm(queries), in_vmem(mine), in_vmem(other), my_docs)


def exchange_x(array):
    return lax.all_to_all(array, "grp", 0, 0, axis_index_groups=OVER_X, tiled=True)


def program(hidden, queries, vis_rows, vis_slot, doc_ids, w_key, w_value):
    tokens = hidden.shape[0]
    cols = 2 * w_key.shape[1]
    grp = lax.axis_index("grp")
    where = jnp.stack([lax.axis_index("seq"), grp // NZ, grp % NZ])
    rows, piece = packed(where, hidden, vis_rows, w_key, w_value)

    got = lax.all_gather(piece, "grp", axis=0, axis_index_groups=OVER_Z)

    rows = exchange_x(rows)

    z = lax.axis_index("grp") % NZ
    far = jnp.stack([lax.dynamic_index_in_dim(got, (z + 1 + i) % NZ, 0, False) for i in range(NZ - 1)])
    far = lax.all_gather(far, "seq", axis=0, axis_index_groups=OVER_NEAR)

    vis, weights = projected_extra(where, rows, w_key, w_value, far)
    vis = exchange_x(vis)
    text = list(projected_text(where, rows, weights))
    for d in (2, 1, 3):
        text[d] = x_permute(text[d], d)
    marks = jnp.broadcast_to(vis_slot.reshape(NS * CAP, 1), (NS * CAP, tokens)).astype(jnp.float32)
    vis = settled(vis, marks)
    vis = lax.all_to_all(vis, "seq", 0, 0, tiled=True)
    docs = jnp.broadcast_to(jnp.tile(doc_ids, (1, cols // tokens)), (8, cols)).astype(jnp.bfloat16)
    block = merged_block(vis, docs, text)

    back = {}
    for d in (2, 3, 1, 4):
        back[d] = seq_permute(back[2] if d == 4 else block, later(2 if d == 4 else d))
    mine = jnp.stack([block, *(back[d] for d in range(1, REACH + 1))])
    other = seq_permute(mine, sibling)
    my_docs = doc_ids.reshape(tokens, 1).astype(jnp.float32)
    return attention(where, queries, mine, other, my_docs)


def solution(mesh):
    return jax.shard_map(
        program,
        mesh=mesh,
        in_specs=(
            P(("grp", "seq"), None),
            P(("grp", "seq"), "tp"),
            P(("grp", "seq"), None, None, None),
            P(("grp", "seq"), None, None),
            P("grp", "seq"),
            P("grp", "tp"),
            P("grp", "tp"),
        ),
        out_specs=P(("grp", "seq"), "tp"),
        check_vma=False,
    )
```

```python
import jax
import jax.numpy as jnp
from jax import lax
from jax.experimental import pallas as pl
from jax.experimental.pallas import tpu as pltpu
from jax.sharding import PartitionSpec as P


HEAD = 128
QPK = 8
CAP = 4
LOG2E = 1.4426950408889634
HEADS_STEP = 4
NX = 4
NZ = 4
NLO = 8
NS = 16
NT = 4
REACH = 4
AXES = ("grp", "seq", "tp")
OVER_X = [[x * NZ + z for x in range(NX)] for z in range(NZ)]
OVER_Z = [[x * NZ + z for z in range(NZ)] for x in range(NX)]
NEAR = 2
OVER_NEAR = [[first + i for i in range(2 * NEAR)] for first in range(0, NS, 2 * NEAR)]


def seq_permute(array, move):
    pairs = []
    for g in range(NX * NZ):
        for s in range(NS):
            to = move(s // 2, s % 2)
            if to is None:
                continue
            for t in range(NT):
                pairs.append(((g * NS + s) * NT + t, (g * NS + to[0] * 2 + to[1]) * NT + t))
    return lax.ppermute(array, AXES, pairs)


def x_permute(array, d):
    step, size = NZ * NS * NT, NX * NZ * NS * NT
    return lax.ppermute(array, AXES, [(i, (i + d * step) % size) for i in range(size)])


def sibling(z, c):
    return z, 1 - c


def later(d):
    return lambda z, c: (z + d, c) if z + d < NLO else None


MIB = 1 << 20
IN_VMEM = pl.BlockSpec(memory_space=pltpu.VMEM)


def whole(shape):
    return pl.BlockSpec(shape, lambda *_: (0,) * len(shape))


def in_vmem(array):
    return pltpu.with_memory_space_constraint(array, pltpu.VMEM)


def in_hbm(array):
    return pltpu.with_memory_space_constraint(array, pltpu.HBM)


def pack(place_ref, text_ref, extra_ref, key_ref, value_ref, out_ref, piece_ref, *scratch):
    extra_in, parts, key_part, value_part, text_sem, in_sem, out_sem, piece_sem = scratch
    tokens = text_ref.shape[0]
    width = out_ref.shape[2]
    part = piece_ref.shape[0]
    s = place_ref[0]
    rows = pl.ds(pl.multiple_of(lax.rem(s // 2, NEAR) * part, part), part)
    pieces = [
        pltpu.make_async_copy(key_ref.at[rows], key_part, piece_sem.at[0]),
        pltpu.make_async_copy(value_ref.at[rows], value_part, piece_sem.at[1]),
    ]
    texts, ins, outs = [], [], []
    for q in range(NX):
        cols = pl.ds(q * width, width)
        ins.append(pltpu.make_async_copy(extra_ref.at[0, :, :, cols], extra_in.at[q], in_sem.at[q]))
        texts.append(
            pltpu.make_async_copy(text_ref.at[:, cols], parts.at[q, pl.ds(0, tokens)], text_sem.at[q])
        )
        outs.append(pltpu.make_async_copy(parts.at[q], out_ref.at[q], out_sem.at[q]))
    for q in range(NX):
        ins[q].start()
        texts[q].start()
    for copy in pieces:
        copy.start()
    for q in range(NX):
        ins[q].wait()
        parts[q, tokens:] = extra_in[q].reshape(NS * CAP, width)
        texts[q].wait()
        outs[q].start()
    for copy in pieces:
        copy.wait()
    piece_ref[...] = jnp.where(lax.rem(s, 2) == 0, key_part[...], value_part[...])
    for copy in outs:
        copy.wait()


def packed(place, hidden, vis_rows, w_key, w_value):
    tokens, width = hidden.shape
    count = tokens + NS * CAP
    part = width // NX
    piece = (w_key.shape[0] // NEAR, w_key.shape[1])
    kind = hidden.dtype
    anywhere = pl.BlockSpec(memory_space=pl.ANY)
    return pl.pallas_call(
        pack,
        grid_spec=pltpu.PrefetchScalarGridSpec(
            num_scalar_prefetch=1,
            grid=(1,),
            in_specs=[anywhere] * 4,
            out_specs=[anywhere, IN_VMEM],
            scratch_shapes=[
                pltpu.VMEM((NX, NS, CAP, part), kind),
                pltpu.VMEM((NX, count, part), kind),
                pltpu.VMEM(piece, kind),
                pltpu.VMEM(piece, kind),
                pltpu.SemaphoreType.DMA((NX,)),
                pltpu.SemaphoreType.DMA((NX,)),
                pltpu.SemaphoreType.DMA((NX,)),
                pltpu.SemaphoreType.DMA((2,)),
            ],
        ),
        out_shape=[pltpu.HBM((NX, count, part), kind), pltpu.VMEM(piece, kind)],
        compiler_params=pltpu.CompilerParams(vmem_limit_bytes=16 * MIB),
        name="pack",
    )(place, *map(in_hbm, (hidden, vis_rows, w_key, w_value)))


def project_extra(
    place_ref, rows_ref, key_ref, value_ref, far_ref, vis_ref, out_ref, weights_ref, in_sem, out_sem
):
    members, sources, part, cols = far_ref.shape
    tokens = rows_ref.shape[1] - NS * CAP
    z = place_ref[2]
    shard = NEAR * part
    own = pl.ds(pl.multiple_of(z * shard, shard), shard)
    copies = [(key_ref, own, 0), (value_ref, own, 1)]
    for i in range(sources):
        first = lax.rem(z + 1 + i, NZ) * shard
        for m in range(members):
            chip, core = divmod(m, 2)
            at = pl.ds(pl.multiple_of(first + chip * part, part), part)
            copies.append((far_ref.at[m, i], at, core))
    copies = [
        pltpu.make_async_copy(
            ref, weights_ref.at[at, pl.ds(side * cols, cols)], in_sem.at[k]
        )
        for k, (ref, at, side) in enumerate(copies)
    ]
    for copy in copies:
        copy.start()
    for copy in copies:
        copy.wait()
    copy = pltpu.make_async_copy(weights_ref, out_ref, out_sem)
    copy.start()
    weights = weights_ref[...]
    for block in range(NX):
        vis_ref[block] = jnp.dot(
            rows_ref[block, tokens:, :], weights, preferred_element_type=jnp.float32
        )
    copy.wait()


def projected_extra(place, rows, w_key, w_value, far):
    blocks, _, part = rows.shape
    cols = 2 * far.shape[-1]
    vis = pltpu.HBM((blocks, NS * CAP, cols), jnp.float32)
    return pl.pallas_call(
        project_extra,
        grid_spec=pltpu.PrefetchScalarGridSpec(
            num_scalar_prefetch=1,
            grid=(1,),
            in_specs=[IN_VMEM] + [pl.BlockSpec(memory_space=pl.ANY)] * 3,
            out_specs=[
                pl.BlockSpec(vis.shape, lambda i, _: (0, 0, 0)),
                pl.BlockSpec(memory_space=pl.ANY),
            ],
            scratch_shapes=[
                pltpu.VMEM((part, cols), jnp.bfloat16),
                pltpu.SemaphoreType.DMA((2 + far.shape[0] * far.shape[1],)),
                pltpu.SemaphoreType.DMA,
            ],
        ),
        out_shape=[vis, pltpu.HBM((part, cols), jnp.bfloat16)],
        compiler_params=pltpu.CompilerParams(vmem_limit_bytes=16 * MIB),
        name="project_extra",
    )(place, in_vmem(rows), in_hbm(w_key), in_hbm(w_value), in_hbm(far))


def project_text(place_ref, rows_ref, weights_ref, own_ref, *text_refs):
    tokens = own_ref.shape[0]
    x = place_ref[1]
    weights = weights_ref[...]
    for d, ref in enumerate((own_ref, *text_refs)):
        ref[...] = jnp.dot(
            rows_ref[lax.rem(x + d, NX), :tokens, :], weights, preferred_element_type=jnp.float32
        )


def projected_text(place, rows, weights):
    blocks, count, _ = rows.shape
    shape = (count - NS * CAP, weights.shape[1])
    return pl.pallas_call(
        project_text,
        grid_spec=pltpu.PrefetchScalarGridSpec(
            num_scalar_prefetch=1,
            grid=(1,),
            in_specs=[IN_VMEM, whole(weights.shape)],
            out_specs=[IN_VMEM] + [pl.BlockSpec(shape, lambda i, _: (0, 0))] * (blocks - 1),
        ),
        out_shape=[pltpu.VMEM(shape, jnp.float32)]
        + [pltpu.HBM(shape, jnp.float32)] * (blocks - 1),
        compiler_params=pltpu.CompilerParams(vmem_limit_bytes=16 * MIB),
        name="project_text",
    )(place, in_vmem(rows), in_hbm(weights))


def settle(sums_ref, marks_ref, out_ref):
    cols = sums_ref.shape[-1]
    rows = (sums_ref[0] + sums_ref[1]) + (sums_ref[2] + sums_ref[3])
    for i in range(NS):
        at = slice(i * CAP, (i + 1) * CAP)
        out_ref[i, :, :cols] = rows[at].astype(jnp.bfloat16)
        out_ref[i, :, cols:] = marks_ref[at, :].astype(jnp.bfloat16)


def settled(sums, marks):
    shape = (NS, CAP, sums.shape[-1] + marks.shape[-1])
    return pl.pallas_call(
        settle,
        grid=(1,),
        in_specs=[IN_VMEM] * 2,
        out_specs=pl.BlockSpec(shape, lambda i: (0, 0, 0)),
        out_shape=pltpu.HBM(shape, jnp.bfloat16),
        compiler_params=pltpu.CompilerParams(vmem_limit_bytes=8 * MIB),
        name="settle",
    )(in_vmem(sums), marks)


def merge(vis_ref, docs_ref, *refs):
    *text_refs, out_ref = refs
    tokens, cols = text_refs[0].shape
    text = (text_refs[0][...] + text_refs[1][...]) + (text_refs[2][...] + text_refs[3][...])
    vis = vis_ref[...].reshape(NS * CAP, vis_ref.shape[-1])
    slots = vis[:, cols:].astype(jnp.float32)
    matches = slots == lax.broadcasted_iota(jnp.int32, slots.shape, 1).astype(jnp.float32)
    chooser = matches.astype(jnp.float32).astype(jnp.bfloat16)
    dims = (((0,), (0,)), ((), ()))
    moved = lax.dot_general(chooser, vis[:, :cols], dims, preferred_element_type=jnp.float32)
    ones = jnp.ones((slots.shape[0], cols), jnp.bfloat16)
    used = lax.dot_general(chooser, ones, dims, preferred_element_type=jnp.float32)
    out_ref[:tokens, :] = jnp.where(used > 0.5, moved, text).astype(jnp.bfloat16)
    out_ref[tokens:, :] = docs_ref[...]


def merged_block(vis, docs, text):
    tokens, cols = text[0].shape
    return pl.pallas_call(
        merge,
        in_specs=[IN_VMEM] * (2 + len(text)),
        out_specs=IN_VMEM,
        out_shape=pltpu.VMEM((tokens + docs.shape[0], cols), jnp.bfloat16),
        compiler_params=pltpu.CompilerParams(vmem_limit_bytes=8 * MIB),
        name="merge",
    )(in_vmem(vis), docs, *map(in_vmem, text))


def attend(place_ref, q_hbm, mine_ref, other_ref, my_docs_ref, out_ref, *scratch):
    bias_ref, keys_ref, values_ref, q_ref, q_sem = scratch
    tokens = q_hbm.shape[0]
    blocks = mine_ref.shape[0]

    @pl.when(pl.program_id(0) == 0)
    def _():
        copy = pltpu.make_async_copy(q_hbm, q_ref, q_sem)
        copy.start()
        s = place_ref[0]
        core, chip = lax.rem(s, 2), s // 2
        my_docs = jnp.broadcast_to(my_docs_ref[...], (tokens, tokens))
        row = lax.broadcasted_iota(jnp.int32, (tokens, tokens), 0) + s * tokens
        col = lax.broadcasted_iota(jnp.int32, (tokens, tokens), 1)
        for side, ref in enumerate((mine_ref, other_ref)):
            for d in range(blocks):
                block = 2 * (chip - d) + (core if side == 0 else 1 - core)
                docs = ref[d, tokens : tokens + 8, :tokens].astype(jnp.float32)[:1]
                spot = col + block * tokens
                allowed = (docs == my_docs) & (spot <= row) & (spot >= 0)
                at = (side * blocks + d) * tokens
                bias_ref[:, at : at + tokens] = jnp.where(allowed, 0.0, -1e30)
                keys_ref[at : at + tokens, :] = ref[d, :tokens, :HEAD]
                values_ref[at : at + tokens, :] = ref[d, :tokens, HEAD:]
        copy.wait()

    scale = jnp.float32(LOG2E) / jnp.sqrt(jnp.float32(HEAD))
    first = pl.multiple_of(pl.program_id(0) * HEADS_STEP * HEAD, HEAD)
    for h in range(HEADS_STEP):
        head = slice(h * HEAD, (h + 1) * HEAD)
        scores = lax.dot_general(
            q_ref[:, pl.ds(first + h * HEAD, HEAD)], keys_ref[...], (((1,), (1,)), ((), ())), preferred_element_type=jnp.float32
        )
        scores = scores * scale + bias_ref[...]
        top = jnp.max(scores, axis=1, keepdims=True)
        weights = jnp.exp2(scores - top)
        total = jnp.sum(weights, axis=1, keepdims=True)
        mixed = jnp.dot(
            weights.astype(jnp.bfloat16), values_ref[...], preferred_element_type=jnp.float32
        )
        out_ref[:, head] = (mixed / total).astype(out_ref.dtype)


def attention(place, queries, mine, other, my_docs):
    tokens = queries.shape[0]
    span = 2 * mine.shape[0] * tokens
    return pl.pallas_call(
        attend,
        grid_spec=pltpu.PrefetchScalarGridSpec(
            num_scalar_prefetch=1,
            grid=(QPK // HEADS_STEP,),
            in_specs=[
                pl.BlockSpec(memory_space=pl.ANY),
                IN_VMEM,
                IN_VMEM,
                IN_VMEM,
            ],
            out_specs=pl.BlockSpec((tokens, HEADS_STEP * HEAD), lambda h, *_: (0, h)),
            scratch_shapes=[
                pltpu.VMEM((tokens, span), jnp.float32),
                pltpu.VMEM((span, HEAD), jnp.bfloat16),
                pltpu.VMEM((span, HEAD), jnp.bfloat16),
                pltpu.VMEM(queries.shape, queries.dtype),
                pltpu.SemaphoreType.DMA,
            ],
        ),
        out_shape=jax.ShapeDtypeStruct(queries.shape, jnp.bfloat16),
        compiler_params=pltpu.CompilerParams(vmem_limit_bytes=16 * MIB),
        name="attend",
    )(place, in_hbm(queries), in_vmem(mine), in_vmem(other), my_docs)


def exchange_x(array):
    return lax.all_to_all(array, "grp", 0, 0, axis_index_groups=OVER_X, tiled=True)


def program(hidden, queries, vis_rows, vis_slot, doc_ids, w_key, w_value):
    tokens = hidden.shape[0]
    cols = 2 * w_key.shape[1]
    grp = lax.axis_index("grp")
    where = jnp.stack([lax.axis_index("seq"), grp // NZ, grp % NZ])
    rows, piece = packed(where, hidden, vis_rows, w_key, w_value)

    got = lax.all_gather(piece, "grp", axis=0, axis_index_groups=OVER_Z)

    rows = exchange_x(rows)

    z = lax.axis_index("grp") % NZ
    far = jnp.stack([lax.dynamic_index_in_dim(got, (z + 1 + i) % NZ, 0, False) for i in range(NZ - 1)])
    far = lax.all_gather(far, "seq", axis=0, axis_index_groups=OVER_NEAR)

    vis, weights = projected_extra(where, rows, w_key, w_value, far)
    vis = exchange_x(vis)
    text = list(projected_text(where, rows, weights))
    for d in (2, 1, 3):
        text[d] = x_permute(text[d], d)
    marks = jnp.broadcast_to(vis_slot.reshape(NS * CAP, 1), (NS * CAP, tokens)).astype(jnp.float32)
    vis = settled(vis, marks)
    vis = lax.all_to_all(vis, "seq", 0, 0, tiled=True)
    docs = jnp.broadcast_to(jnp.tile(doc_ids, (1, cols // tokens)), (8, cols)).astype(jnp.bfloat16)
    block = merged_block(vis, docs, text)

    back = {0: block}
    for d in (2, 1, 4, 3):
        back[d] = seq_permute(back[max(d - 2, 0)], later(min(d, 2)))
    mine = jnp.stack([block, *(back[d] for d in range(1, REACH + 1))])
    other = seq_permute(mine, sibling)
    my_docs = doc_ids.reshape(tokens, 1).astype(jnp.float32)
    return attention(where, queries, mine, other, my_docs)


def solution(mesh):
    return jax.shard_map(
        program,
        mesh=mesh,
        in_specs=(
            P(("grp", "seq"), None),
            P(("grp", "seq"), "tp"),
            P(("grp", "seq"), None, None, None),
            P(("grp", "seq"), None, None),
            P("grp", "seq"),
            P("grp", "tp"),
            P("grp", "tp"),
        ),
        out_specs=P(("grp", "seq"), "tp"),
        check_vma=False,
    )
```
